128 devices in a mesh: row: 16 (over y, x_hi, core), col: 8 (over x_lo, z).
Axes of the slice: x: 4 (x_hi: 2, x_lo: 2; x = x_hi * 2 + x_lo), y: 4, z: 4, core: 2. Of those that a mesh axis runs over, the one named last changes fastest.
Arguments:
- sqrt_iterate: float32 [256, 128, 1024], P(('row', 'col'))
- inverse_iterate: float32 [256, 128, 1024], P(('row', 'col'))
- pattern: int32 [256, 8], replicated, may hold values from 0 to 255, as said below
- keep_mask: int32 [256, 8], replicated, may hold values 0 or 1
- row_order: int32 [256], replicated, may hold values from 0 to 255, as said below
Outputs:
- sqrt_next: float32 [256, 128, 1024], P(('row', 'col'))
- inverse_next: float32 [256, 128, 1024], P(('row', 'col'))
The draws below stay inside these ranges and needn't reach their ends.
Inputs may be any that keep to these rules, and one draw needn't show every extreme that they name: row_order holds each of 0 to 255 once. pattern[s, 0] = row_order[s]; the labels of one row are distinct; each label in row s is that of a block row stored on the same device as s, on one of the two devices one step away along row (wrapping), or on the next device along col (wrapping). Stored position s lies on device index (s // 2) in the order of the mesh with row slowest.
All inputs are finite; a program needn't handle non-finite values.
Results may differ from the reference program's by a relative error of at most 0.00011.
Values sent between devices are 32-bit elements; how exact they have to be, the bound alone decides.
A program may use at most 128 MiB of HBM per device.

```python
import jax
import jax.numpy as jnp
from jax import lax

BLOCK = 128
SLOTS = 8
ROWS_DEV = 2
NBLK = 256
N_ROW = 16
N_COL = 8


def shared_order(key):
    return jax.random.permutation(jax.random.fold_in(key, 11), NBLK).astype(jnp.int32)


def draw_row_order(key, part):
    return shared_order(key)


def draw_pattern(key, part):
    ordering = shared_order(key)
    row_ids = jnp.arange(NBLK, dtype=jnp.int32)
    candidates = 4 * ROWS_DEV
    cand_ids = jnp.arange(candidates, dtype=jnp.int32)
    scores = jax.random.randint(jax.random.fold_in(key, 12), (NBLK, candidates), 0, 2 ** 20) * candidates + cand_ids[None, :]
    self_cand = ROWS_DEV + row_ids % ROWS_DEV
    scores = jnp.where(cand_ids[None, :] == self_cand[:, None], -1, scores)
    unused, chosen_ids = lax.top_k(scores, SLOTS - 1)
    region = chosen_ids // ROWS_DEV
    offset = chosen_ids % ROWS_DEV
    device = row_ids // ROWS_DEV
    row_of = (device // N_COL)[:, None]
    col_of = (device % N_COL)[:, None]
    prev_dev = (row_of + N_ROW - 1) % N_ROW * N_COL + col_of
    next_dev = (row_of + 1) % N_ROW * N_COL + col_of
    own_dev = row_of * N_COL + col_of
    side_dev = row_of * N_COL + (col_of + 1) % N_COL
    target = jnp.where(region == 0, prev_dev, jnp.where(region == 1, own_dev, jnp.where(region == 2, next_dev, side_dev)))
    position = (target * ROWS_DEV + offset).astype(jnp.int32)
    columns_all = jnp.concatenate([row_ids[:, None], position], axis=1)
    return ordering[columns_all]


def block_matrix(key):
    full_shape = (NBLK, BLOCK, SLOTS * BLOCK)
    random_part = jax.random.normal(key, full_shape, jnp.float32)
    identity = (jnp.arange(SLOTS * BLOCK)[None, :] == jnp.arange(BLOCK)[:, None]).astype(jnp.float32)
    return 0.7 / BLOCK ** 0.5 * random_part + identity[None]


def draw_sqrt_iterate(key, part):
    return block_matrix(jax.random.fold_in(key, 21))


def draw_inverse_iterate(key, part):
    return block_matrix(jax.random.fold_in(key, 22))


def touch_ends(drawn, key, smallest, top_value):
    longest = drawn.shape.index(max(drawn.shape))
    spots = []
    for shift in (0, 1):
        where = [jax.random.randint(jax.random.fold_in(key, axis), (), 0, length) for axis, length in enumerate(drawn.shape)]
        where[longest] = (where[longest] + shift) % drawn.shape[longest]
        spots.append(tuple(where))
    return drawn.at[spots[0]].set(smallest).at[spots[1]].set(top_value)


def setup_inputs(seed: int = 0) -> dict:
    seeds = jax.random.split(jax.random.key(seed), 6)
    sqrt_iterate = draw_sqrt_iterate(jax.random.fold_in(seeds[5], 71), 0)
    inverse_iterate = draw_inverse_iterate(jax.random.fold_in(seeds[5], 71), 0)
    pattern = draw_pattern(jax.random.fold_in(seeds[5], 71), 0)
    keep_mask = touch_ends((jax.random.randint(seeds[3], (NBLK, SLOTS), 0, 4) < 3).astype(jnp.int32), jax.random.fold_in(seeds[3], 1), 0, 1)
    row_order = draw_row_order(jax.random.fold_in(seeds[5], 71), 0)
    return dict(sqrt_iterate=sqrt_iterate, inverse_iterate=inverse_iterate, pattern=pattern, keep_mask=keep_mask, row_order=row_order)


PRECISE = lax.Precision.HIGHEST

def filtered_product(left_factor, right_factor, position, selector, kept_cols):
    block_rows, block_size, row_width = left_factor.shape
    slot_count = row_width // block_size

    def row_product(row_items):
        row_block, positions, row_selector, keep_row = row_items
        picked = right_factor[positions].reshape(slot_count, block_size, slot_count, block_size)
        chosen = jnp.einsum('kimj,kpm->kipj', picked, row_selector, precision=PRECISE)
        chosen = chosen.reshape(row_width, row_width)
        return jnp.dot(row_block, chosen, precision=PRECISE, preferred_element_type=jnp.float32) * keep_row
    return lax.map(row_product, (left_factor, position, selector, kept_cols))

def reference(sqrt_iterate, inverse_iterate, pattern, keep_mask, row_order):
    block_rows, block_size, row_width = sqrt_iterate.shape
    slot_count = row_width // block_size
    inverse_order = jnp.zeros((block_rows,), jnp.int32).at[row_order].set(jnp.arange(block_rows, dtype=jnp.int32))
    position = inverse_order[pattern]
    selector = (pattern[position][:, :, None, :] == pattern[:, None, :, None]).astype(jnp.float32)
    slot_ids = jnp.arange(slot_count, dtype=jnp.int32)
    kept = jnp.maximum(keep_mask, (slot_ids == 0).astype(jnp.int32)[None, :])
    kept_cols = jnp.repeat(kept.astype(jnp.float32), block_size, axis=1)[:, None, :]
    identity = (jnp.arange(row_width)[None, :] == jnp.arange(block_size)[:, None]).astype(jnp.float32)
    product = filtered_product(inverse_iterate, sqrt_iterate, position, selector, kept_cols)
    factor = 1.5 * identity[None] - 0.5 * product
    sqrt_next = filtered_product(sqrt_iterate, factor, position, selector, kept_cols)
    inverse_next = filtered_product(factor, inverse_iterate, position, selector, kept_cols)
    return (sqrt_next, inverse_next)
```

```python
import functools

import jax
import jax.numpy as jnp
from jax import lax
from jax.experimental import pallas as pl
from jax.experimental.pallas import tpu as pltpu
from jax.sharding import PartitionSpec as P

MESH = pl.DeviceIdType.MESH
BLK = 128
ROWS = 2
SLOTS = 8
UNIT = ROWS * BLK

OWN, NEAR, FAR, SIDE = 0, 1, 2, 3

(Y_NO, Y_NN, Z_NO, Z_NN, T_NO, T_NN,
 Y_XO, Y_XX, Z_XO, Z_XX, T_XX,
 Y_SS, Z_SS, T_SS) = range(14)


def split(value):
    high = value.astype(jnp.bfloat16)
    low = (value - high.astype(jnp.float32)).astype(jnp.bfloat16)
    return high, low


def kernel(row_count, col_count, pat_ref, keep_ref, y_ref, z_ref, yn_ref, zn_ref,
           own_y, own_z, own_t, recv, yh, yl, zh, zl, th, tl, rh, rl, acc_y, acc_z,
           send_sem, recv_sem):
    row = lax.axis_index("row")
    col = lax.axis_index("col")
    odd = lax.rem(row, 2)
    near = (row + 1 - 2 * odd, col)
    far = (lax.rem(row + row_count - 1 + 2 * odd, row_count), col)
    side = (row, lax.rem(col + 1, col_count))
    back = (row, lax.rem(col + col_count - 1, col_count))

    barrier = pltpu.get_barrier_semaphore()
    for other in (near, far, side, back):
        pl.semaphore_signal(barrier, inc=1, device_id=other, device_id_type=MESH)

    def first(place):
        return (place[0] * col_count + place[1]) * ROWS

    starts = [first(place) for place in ((row, col), near, far, side)]
    labels = [pat_ref[0, starts[q // ROWS] + q % ROWS] for q in range(SLOTS)]

    def pick(wanted, keys, values):
        found = values[0]
        for key, value in zip(keys[1:], values[1:]):
            found = jnp.where(key == wanted, value, found)
        return found

    numbers = [jnp.int32(k) for k in range(SLOTS)]
    keys = [[pat_ref[k, starts[OWN] + s] for k in range(SLOTS)] for s in range(ROWS)]
    keep = [[jnp.float32(1)] + [keep_ref[k, starts[OWN] + s].astype(jnp.float32) for k in range(1, SLOTS)]
            for s in range(ROWS)]
    slot_of = [[pick(labels[q], keys[s], numbers) for q in range(SLOTS)] for s in range(ROWS)]
    place_of = [[pick(keys[s][k], labels, numbers) for k in range(SLOTS)] for s in range(ROWS)]
    kept = [[pick(labels[q], keys[s], keep[s]) for q in range(SLOTS)] for s in range(ROWS)]
    kept_far = []
    for s in range(ROWS):
        far_keys = [pat_ref[k, starts[FAR] + s] for k in range(SLOTS)]
        far_keep = [keep_ref[k, starts[FAR] + s].astype(jnp.float32) for k in range(SLOTS)]
        kept_far.append([pick(labels[e], far_keys, far_keep) for e in range(ROWS)])

    def same(value, number):
        return jnp.full((BLK, BLK), value, jnp.int32) == number

    def blk(s, e):
        return pl.ds(s * BLK, BLK), pl.ds(e * BLK, BLK)

    for source, whole, high, low in ((y_ref, own_y, yh, yl), (z_ref, own_z, zh, zl)):
        for g in range(4):
            for s in range(ROWS):
                for e in range(ROWS):
                    slot = slot_of[s][g * ROWS + e]
                    value = source[s, :, pl.ds(0, BLK)]
                    for k in range(1, SLOTS):
                        value = jnp.where(same(slot, k), source[s, :, pl.ds(k * BLK, BLK)], value)
                    h, l = split(value)
                    where = (g, *blk(s, e))
                    whole[where] = value
                    high[where] = h
                    low[where] = l

    pl.semaphore_wait(barrier, 4)

    copies = {}

    def send(source, unit, target):
        copy = pltpu.make_async_remote_copy(
            src_ref=source, dst_ref=recv.at[unit], send_sem=send_sem.at[unit],
            recv_sem=recv_sem.at[unit], device_id=target, device_id_type=MESH)
        copy.start()
        copies[unit] = copy

    send(own_y.at[FAR], Y_XO, far)
    send(own_y.at[OWN], Y_SS, back)
    send(own_y.at[NEAR], Y_NO, near)
    send(own_y.at[OWN], Y_XX, far)
    send(own_z.at[OWN], Z_SS, back)
    send(own_y.at[OWN], Y_NN, near)
    send(own_z.at[FAR], Z_XO, far)
    send(own_z.at[NEAR], Z_NO, near)
    send(own_z.at[OWN], Z_XX, far)
    send(own_z.at[OWN], Z_NN, near)

    def arrive(unit):
        copies[unit].wait_recv()
        h, l = split(recv[unit])
        rh[unit] = h
        rl[unit] = l

    def mul(a_high, a_low, b_high, b_low):
        dot = functools.partial(jnp.dot, preferred_element_type=jnp.float32)
        return dot(a_high, b_high) + (dot(a_high, b_low) + dot(a_low, b_high))

    Y = lambda g: (yh[g], yl[g])
    Z = lambda g: (zh[g], zl[g])
    T = lambda g: (th[g], tl[g])
    R = lambda u: (rh[u], rl[u])

    def factor_of(product, region, s, e):
        value = (-0.5 * kept[s][region * ROWS + e]) * product[s * BLK:(s + 1) * BLK, e * BLK:(e + 1) * BLK]
        if region == OWN and s == e:
            eye = lax.broadcasted_iota(jnp.int32, (BLK, BLK), 0) == lax.broadcasted_iota(jnp.int32, (BLK, BLK), 1)
            value = value + jnp.where(eye, jnp.float32(1.5), jnp.float32(0))
        return value

    def set_factor(region, product):
        for s in range(ROWS):
            for e in range(ROWS):
                value = factor_of(product, region, s, e)
                h, l = split(value)
                where = (region, *blk(s, e))
                th[where] = h
                tl[where] = l
                if region in (OWN, NEAR):
                    own_t[where] = value

    def parts(g):
        return [(g * ROWS + e, s, blk_of(s, e)) for s in range(ROWS) for e in range(ROWS)]

    def blk_of(s, e):
        return slice(s * BLK, (s + 1) * BLK), slice(e * BLK, (e + 1) * BLK)

    def put(acc, g, value):
        for q, s, where in parts(g):
            acc[q, s] = value[where]

    def add(acc, g, value):
        for q, s, where in parts(g):
            acc[q, s] += value[where]

    def get(acc, g):
        rows = [jnp.concatenate([acc[g * ROWS + e, s] for e in range(ROWS)], axis=1) for s in range(ROWS)]
        return jnp.concatenate(rows, axis=0)

    arrive(Y_NO)
    put(acc_z, OWN, mul(*Z(OWN), *Y(OWN)) + mul(*Z(NEAR), *R(Y_NO)))
    arrive(Y_NN)
    set_factor(NEAR, mul(*Z(OWN), *Y(NEAR)) + mul(*Z(NEAR), *R(Y_NN)))
    send(own_t.at[NEAR], T_NO, near)
    put(acc_z, FAR, mul(*Z(OWN), *Y(FAR)))
    put(acc_z, SIDE, mul(*Z(OWN), *Y(SIDE)))
    put(acc_y, NEAR, mul(*Y(OWN), *T(NEAR)))
    arrive(Y_XO)
    set_factor(OWN, get(acc_z, OWN) + mul(*Z(FAR), *R(Y_XO)))
    arrive(Z_NO)
    arrive(Z_NN)
    send(own_t.at[OWN], T_XX, far)
    send(own_t.at[OWN], T_SS, back)
    send(own_t.at[OWN], T_NN, near)
    put(acc_y, OWN, mul(*Y(OWN), *T(OWN)))
    put(acc_z, OWN, mul(*T(OWN), *Z(OWN)) + mul(*T(NEAR), *R(Z_NO)))
    put(acc_z, NEAR, mul(*T(OWN), *Z(NEAR)) + mul(*T(NEAR), *R(Z_NN)))
    arrive(T_NO)
    add(acc_y, OWN, mul(*Y(NEAR), *R(T_NO)))
    arrive(Y_SS)
    set_factor(SIDE, get(acc_z, SIDE) + mul(*Z(SIDE), *R(Y_SS)))
    put(acc_z, SIDE, mul(*T(OWN), *Z(SIDE)))
    put(acc_y, SIDE, mul(*Y(OWN), *T(SIDE)))
    arrive(T_NN)
    add(acc_y, NEAR, mul(*Y(NEAR), *R(T_NN)))
    arrive(Y_XX)
    set_factor(FAR, get(acc_z, FAR) + mul(*Z(FAR), *R(Y_XX)))
    put(acc_z, FAR, mul(*T(OWN), *Z(FAR)))
    put(acc_y, FAR, mul(*Y(OWN), *T(FAR)))
    arrive(Z_SS)
    add(acc_z, SIDE, mul(*T(SIDE), *R(Z_SS)))
    arrive(Z_XO)
    add(acc_z, OWN, mul(*T(FAR), *R(Z_XO)))
    arrive(Z_XX)
    add(acc_z, FAR, mul(*T(FAR), *R(Z_XX)))
    other = mul(*R(Z_XX), *R(Y_XO)) + mul(*R(Z_XO), *Y(OWN))
    for s in range(ROWS):
        for e in range(ROWS):
            value = (-0.5 * kept_far[s][e]) * other[s * BLK:(s + 1) * BLK, e * BLK:(e + 1) * BLK]
            h, l = split(value)
            rh[(Z_XX, *blk(s, e))] = h
            rl[(Z_XX, *blk(s, e))] = l
    add(acc_y, OWN, mul(*Y(FAR), *R(Z_XX)))

    def emit(result, out):
        for s in range(ROWS):
            for p in range(SLOTS):
                out[s, :, pl.ds(p * BLK, BLK)] = keep[s][p] * result[place_of[s][p], s]

    emit(acc_z, zn_ref)
    arrive(T_SS)
    add(acc_y, SIDE, mul(*Y(SIDE), *R(T_SS)))
    arrive(T_XX)
    add(acc_y, FAR, mul(*Y(FAR), *R(T_XX)))
    emit(acc_y, yn_ref)
    for copy in copies.values():
        copy.wait_send()


def local(row_count, col_count, sqrt_iterate, inverse_iterate, pattern, keep_mask, row_order):
    del row_order
    whole = jax.ShapeDtypeStruct(sqrt_iterate.shape, jnp.float32)
    unit = (UNIT, UNIT)
    vmem = pl.BlockSpec(memory_space=pltpu.VMEM)
    smem = pl.BlockSpec(memory_space=pltpu.SMEM)
    f32 = lambda n: pltpu.VMEM((n, *unit), jnp.float32)
    b16 = lambda n: pltpu.VMEM((n, *unit), jnp.bfloat16)
    return pl.pallas_call(
        functools.partial(kernel, row_count, col_count),
        out_shape=(whole, whole),
        in_specs=[smem, smem, vmem, vmem],
        out_specs=(vmem, vmem),
        scratch_shapes=[
            f32(4), f32(4), f32(2), f32(14),
            b16(4), b16(4), b16(4), b16(4), b16(4), b16(4), b16(14), b16(14),
            pltpu.VMEM((SLOTS, ROWS, BLK, BLK), jnp.float32),
            pltpu.VMEM((SLOTS, ROWS, BLK, BLK), jnp.float32),
            pltpu.SemaphoreType.DMA((14,)),
            pltpu.SemaphoreType.DMA((14,)),
        ],
        compiler_params=pltpu.CompilerParams(
            collective_id=0, has_side_effects=True, vmem_limit_bytes=48 << 20),
    )(pattern.T, keep_mask.T, sqrt_iterate, inverse_iterate)


def solution(mesh):
    split_rows = P(("row", "col"), None, None)
    body = functools.partial(local, mesh.shape["row"], mesh.shape["col"])
    return jax.shard_map(
        body, mesh=mesh, in_specs=(split_rows, split_rows, P(), P(), P()),
        out_specs=(split_rows, split_rows), check_vma=False)
```

```python
import functools

import jax
import jax.numpy as jnp
from jax import lax
from jax.experimental import pallas as pl
from jax.experimental.pallas import tpu as pltpu
from jax.sharding import PartitionSpec as P

MESH = pl.DeviceIdType.MESH
BLK = 128
ROWS = 2
SLOTS = 8
UNIT = ROWS * BLK

OWN, NEAR, FAR, SIDE = 0, 1, 2, 3

RUN = 4
CHUNK = UNIT // RUN

(Y_NO, Y_NN, Z_NO, Z_NN, T_NO, T_NN,
 Y_XO, Y_XX, Z_XO, Z_XX, T_XX,
 Y_SS, Z_SS, T_SS) = range(14)
SIDES = (Y_SS, Z_SS, T_SS)


def split(value):
    high = value.astype(jnp.bfloat16)
    low = (value - high.astype(jnp.float32)).astype(jnp.bfloat16)
    return high, low


def kernel(row_count, col_count, pat_hbm, keep_hbm, y_hbm, z_hbm, yn_ref, zn_ref,
           pat_ref, keep_ref, y_ref, z_ref,
           own_y, own_z, own_t, recv, relay, yh, yl, zh, zl, th, tl, rh, rl, acc_y, acc_z,
           send_sem, recv_sem, side_send, side_recv, relay_send, relay_recv, load_sem):
    loads = [
        pltpu.make_async_copy(source, target, load_sem.at[i])
        for i, (source, target) in enumerate((
            (pat_hbm, pat_ref), (keep_hbm, keep_ref), (y_hbm, y_ref), (z_hbm, z_ref)))
    ]
    for load in loads:
        load.start()
    row = lax.axis_index("row")
    col = lax.axis_index("col")
    odd = lax.rem(row, 2)
    near = (row + 1 - 2 * odd, col)
    far = (lax.rem(row + row_count - 1 + 2 * odd, row_count), col)
    side = (row, lax.rem(col + 1, col_count))
    back = (row, lax.rem(col + col_count - 1, col_count))
    place = lax.rem(col, RUN)
    wrap = (row, lax.rem(col - place + col_count - 1, col_count))

    barrier = pltpu.get_barrier_semaphore()
    peers = [(row, lax.rem(col + d, col_count)) for d in range(1, col_count)]
    for other in [near, far] + peers:
        pl.semaphore_signal(barrier, inc=1, device_id=other, device_id_type=MESH)
    loads[0].wait()
    loads[1].wait()

    def first(place):
        return (place[0] * col_count + place[1]) * ROWS

    starts = [first(place) for place in ((row, col), near, far, side)]
    labels = [pat_ref[0, starts[q // ROWS] + q % ROWS] for q in range(SLOTS)]

    def pick(wanted, keys, values):
        found = values[0]
        for key, value in zip(keys[1:], values[1:]):
            found = jnp.where(key == wanted, value, found)
        return found

    numbers = [jnp.int32(k) for k in range(SLOTS)]
    keys = [[pat_ref[k, starts[OWN] + s] for k in range(SLOTS)] for s in range(ROWS)]
    keep = [[jnp.float32(1)] + [keep_ref[k, starts[OWN] + s].astype(jnp.float32) for k in range(1, SLOTS)]
            for s in range(ROWS)]
    slot_of = [[pick(labels[q], keys[s], numbers) for q in range(SLOTS)] for s in range(ROWS)]
    place_of = [[pick(keys[s][k], labels, numbers) for k in range(SLOTS)] for s in range(ROWS)]
    kept = [[pick(labels[q], keys[s], keep[s]) for q in range(SLOTS)] for s in range(ROWS)]
    kept_far = []
    for s in range(ROWS):
        far_keys = [pat_ref[k, starts[FAR] + s] for k in range(SLOTS)]
        far_keep = [keep_ref[k, starts[FAR] + s].astype(jnp.float32) for k in range(SLOTS)]
        kept_far.append([pick(labels[e], far_keys, far_keep) for e in range(ROWS)])

    def same(value, number):
        return jnp.full((BLK, BLK), value, jnp.int32) == number

    def blk(s, e):
        return pl.ds(s * BLK, BLK), pl.ds(e * BLK, BLK)

    for load, source, whole, high, low in (
            (loads[2], y_ref, own_y, yh, yl), (loads[3], z_ref, own_z, zh, zl)):
        load.wait()
        for g in range(4):
            for s in range(ROWS):
                for e in range(ROWS):
                    slot = slot_of[s][g * ROWS + e]
                    value = source[s, :, pl.ds(0, BLK)]
                    for k in range(1, SLOTS):
                        value = jnp.where(same(slot, k), source[s, :, pl.ds(k * BLK, BLK)], value)
                    h, l = split(value)
                    where = (g, *blk(s, e))
                    whole[where] = value
                    high[where] = h
                    low[where] = l

    pl.semaphore_wait(barrier, 1 + col_count)

    copies = {}

    def send(source, unit, target):
        copy = pltpu.make_async_remote_copy(
            src_ref=source, dst_ref=recv.at[unit], send_sem=send_sem.at[unit],
            recv_sem=recv_sem.at[unit], device_id=target, device_id_type=MESH)
        copy.start()
        copies[unit] = copy

    def chunk(j):
        return pl.ds(j * CHUNK, CHUNK)

    def side_copy(source, number, j):
        return pltpu.make_async_remote_copy(
            src_ref=source.at[chunk(j)], dst_ref=recv.at[SIDES[number], chunk(j)],
            send_sem=side_send.at[number, j], recv_sem=side_recv.at[number, j],
            device_id=back, device_id_type=MESH)

    def detour_copy(source, number, j):
        return pltpu.make_async_remote_copy(
            src_ref=source.at[chunk(j)], dst_ref=relay.at[number],
            send_sem=side_send.at[number, j], recv_sem=relay_recv.at[number],
            device_id=(row, col + j), device_id_type=MESH)

    def relay_copy(number):
        return pltpu.make_async_remote_copy(
            src_ref=relay.at[number], dst_ref=recv.at[SIDES[number], chunk(place)],
            send_sem=relay_send.at[number], recv_sem=side_recv.at[number, place],
            device_id=wrap, device_id_type=MESH)

    def send_side(source, number):
        @pl.when(place == 0)
        def _():
            for j in range(1, RUN):
                detour_copy(source, number, j).start()

        side_copy(source, number, 0).start()

        @pl.when(place != 0)
        def _():
            for j in range(1, RUN):
                side_copy(source, number, j).start()

    def pass_on(number):
        @pl.when(place != 0)
        def _():
            pltpu.make_async_remote_copy(
                src_ref=own_y.at[OWN, chunk(0)], dst_ref=relay.at[number],
                send_sem=side_send.at[number, 0], recv_sem=relay_recv.at[number],
                device_id=back, device_id_type=MESH).wait_recv()
            relay_copy(number).start()

    send(own_y.at[FAR], Y_XO, far)
    send(own_y.at[OWN], Y_XX, far)
    send(own_z.at[FAR], Z_XO, far)
    send(own_z.at[OWN], Z_XX, far)
    send(own_y.at[NEAR], Y_NO, near)
    send(own_y.at[OWN], Y_NN, near)
    send_side(own_y.at[OWN], 0)
    send_side(own_z.at[OWN], 1)
    send(own_z.at[NEAR], Z_NO, near)
    send(own_z.at[OWN], Z_NN, near)

    def arrive(unit):
        if unit in SIDES:
            number = SIDES.index(unit)
            for j in range(RUN):
                side_copy(own_y.at[OWN], number, j).wait_recv()
        else:
            copies[unit].wait_recv()
        h, l = split(recv[unit])
        rh[unit] = h
        rl[unit] = l

    def mul(a_high, a_low, b_high, b_low):
        dot = functools.partial(jnp.dot, preferred_element_type=jnp.float32)
        return dot(a_high, b_high) + (dot(a_high, b_low) + dot(a_low, b_high))

    Y = lambda g: (yh[g], yl[g])
    Z = lambda g: (zh[g], zl[g])
    T = lambda g: (th[g], tl[g])
    R = lambda u: (rh[u], rl[u])

    def factor_of(product, region, s, e):
        value = (-0.5 * kept[s][region * ROWS + e]) * product[s * BLK:(s + 1) * BLK, e * BLK:(e + 1) * BLK]
        if region == OWN and s == e:
            eye = lax.broadcasted_iota(jnp.int32, (BLK, BLK), 0) == lax.broadcasted_iota(jnp.int32, (BLK, BLK), 1)
            value = value + jnp.where(eye, jnp.float32(1.5), jnp.float32(0))
        return value

    def set_factor(region, product):
        for s in range(ROWS):
            for e in range(ROWS):
                value = factor_of(product, region, s, e)
                h, l = split(value)
                where = (region, *blk(s, e))
                th[where] = h
                tl[where] = l
                if region in (OWN, NEAR):
                    own_t[where] = value

    def parts(g):
        return [(g * ROWS + e, s, blk_of(s, e)) for s in range(ROWS) for e in range(ROWS)]

    def blk_of(s, e):
        return slice(s * BLK, (s + 1) * BLK), slice(e * BLK, (e + 1) * BLK)

    def put(acc, g, value):
        for q, s, where in parts(g):
            acc[q, s] = value[where]

    def add(acc, g, value):
        for q, s, where in parts(g):
            acc[q, s] += value[where]

    def get(acc, g):
        rows = [jnp.concatenate([acc[g * ROWS + e, s] for e in range(ROWS)], axis=1) for s in range(ROWS)]
        return jnp.concatenate(rows, axis=0)

    arrive(Y_NO)
    put(acc_z, OWN, mul(*Z(OWN), *Y(OWN)) + mul(*Z(NEAR), *R(Y_NO)))
    arrive(Y_NN)
    set_factor(NEAR, mul(*Z(OWN), *Y(NEAR)) + mul(*Z(NEAR), *R(Y_NN)))
    send(own_t.at[NEAR], T_NO, near)
    put(acc_z, FAR, mul(*Z(OWN), *Y(FAR)))
    put(acc_z, SIDE, mul(*Z(OWN), *Y(SIDE)))
    put(acc_y, NEAR, mul(*Y(OWN), *T(NEAR)))
    pass_on(0)
    pass_on(1)
    arrive(Y_XO)
    set_factor(OWN, get(acc_z, OWN) + mul(*Z(FAR), *R(Y_XO)))
    arrive(Z_NO)
    arrive(Z_NN)
    send(own_t.at[OWN], T_XX, far)
    send_side(own_t.at[OWN], 2)
    send(own_t.at[OWN], T_NN, near)
    put(acc_y, OWN, mul(*Y(OWN), *T(OWN)))
    put(acc_z, OWN, mul(*T(OWN), *Z(OWN)) + mul(*T(NEAR), *R(Z_NO)))
    put(acc_z, NEAR, mul(*T(OWN), *Z(NEAR)) + mul(*T(NEAR), *R(Z_NN)))
    arrive(T_NO)
    add(acc_y, OWN, mul(*Y(NEAR), *R(T_NO)))
    pass_on(2)
    arrive(T_NN)
    add(acc_y, NEAR, mul(*Y(NEAR), *R(T_NN)))
    arrive(Y_XX)
    set_factor(FAR, get(acc_z, FAR) + mul(*Z(FAR), *R(Y_XX)))
    put(acc_z, FAR, mul(*T(OWN), *Z(FAR)))
    put(acc_y, FAR, mul(*Y(OWN), *T(FAR)))
    arrive(Z_XO)
    add(acc_z, OWN, mul(*T(FAR), *R(Z_XO)))
    arrive(Y_SS)
    set_factor(SIDE, get(acc_z, SIDE) + mul(*Z(SIDE), *R(Y_SS)))
    put(acc_z, SIDE, mul(*T(OWN), *Z(SIDE)))
    put(acc_y, SIDE, mul(*Y(OWN), *T(SIDE)))
    arrive(Z_SS)
    add(acc_z, SIDE, mul(*T(SIDE), *R(Z_SS)))
    arrive(Z_XX)
    add(acc_z, FAR, mul(*T(FAR), *R(Z_XX)))
    other = mul(*R(Z_XX), *R(Y_XO)) + mul(*R(Z_XO), *Y(OWN))
    for s in range(ROWS):
        for e in range(ROWS):
            value = (-0.5 * kept_far[s][e]) * other[s * BLK:(s + 1) * BLK, e * BLK:(e + 1) * BLK]
            h, l = split(value)
            rh[(Z_XX, *blk(s, e))] = h
            rl[(Z_XX, *blk(s, e))] = l
    add(acc_y, OWN, mul(*Y(FAR), *R(Z_XX)))

    def emit(result, out):
        for s in range(ROWS):
            for p in range(SLOTS):
                out[s, :, pl.ds(p * BLK, BLK)] = keep[s][p] * result[place_of[s][p], s]

    emit(acc_z, zn_ref)
    arrive(T_SS)
    add(acc_y, SIDE, mul(*Y(SIDE), *R(T_SS)))
    arrive(T_XX)
    add(acc_y, FAR, mul(*Y(FAR), *R(T_XX)))
    emit(acc_y, yn_ref)
    for copy in copies.values():
        copy.wait_send()
    for number in range(len(SIDES)):
        for j in range(RUN):
            side_copy(own_y.at[OWN], number, j).wait_send()

    @pl.when(place != 0)
    def _():
        for number in range(len(SIDES)):
            relay_copy(number).wait_send()


def write_out(y_ref, z_ref, y_hbm, z_hbm, sem):
    copies = []
    for source, target in ((y_ref, y_hbm), (z_ref, z_hbm)):
        for s in range(ROWS):
            for part in range(2):
                where = (s, pl.ds(part * (BLK // 2), BLK // 2))
                copies.append(pltpu.make_async_copy(source.at[where], target.at[where], sem.at[len(copies)]))
    for copy in copies:
        copy.start()
    for copy in copies:
        copy.wait()


def local(row_count, col_count, sqrt_iterate, inverse_iterate, pattern, keep_mask, row_order):
    del row_order
    whole = jax.ShapeDtypeStruct(sqrt_iterate.shape, jnp.float32)
    unit = (UNIT, UNIT)
    vmem = pl.BlockSpec(memory_space=pltpu.VMEM)
    f32 = lambda n: pltpu.VMEM((n, *unit), jnp.float32)
    b16 = lambda n: pltpu.VMEM((n, *unit), jnp.bfloat16)
    hbm = pl.BlockSpec(memory_space=pltpu.HBM)
    dma = pltpu.SemaphoreType.DMA
    results = pl.pallas_call(
        functools.partial(kernel, row_count, col_count),
        out_shape=(whole, whole),
        in_specs=[hbm] * 4,
        out_specs=(vmem, vmem),
        scratch_shapes=[
            pltpu.SMEM(pattern.shape[::-1], jnp.int32), pltpu.SMEM(pattern.shape[::-1], jnp.int32),
            pltpu.VMEM(whole.shape, jnp.float32), pltpu.VMEM(whole.shape, jnp.float32),
            f32(4), f32(4), f32(2), f32(14), pltpu.VMEM((len(SIDES), CHUNK, UNIT), jnp.float32),
            b16(4), b16(4), b16(4), b16(4), b16(4), b16(4), b16(14), b16(14),
            pltpu.VMEM((SLOTS, ROWS, BLK, BLK), jnp.float32),
            pltpu.VMEM((SLOTS, ROWS, BLK, BLK), jnp.float32),
            dma((14,)), dma((14,)), dma((len(SIDES), RUN)), dma((len(SIDES), RUN)),
            dma((len(SIDES),)), dma((len(SIDES),)), dma((4,)),
        ],
        compiler_params=pltpu.CompilerParams(
            collective_id=0, has_side_effects=True, vmem_limit_bytes=54_000_000),
    )(pattern.T, keep_mask.T, sqrt_iterate, inverse_iterate)
    return pl.pallas_call(
        write_out,
        out_shape=(whole, whole),
        in_specs=[vmem, vmem],
        out_specs=(hbm, hbm),
        scratch_shapes=[dma((8,))],
        compiler_params=pltpu.CompilerParams(vmem_limit_bytes=4194304),
    )(*results)


def solution(mesh):
    split_rows = P(("row", "col"), None, None)
    body = functools.partial(local, mesh.shape["row"], mesh.shape["col"])
    return jax.shard_map(
        body, mesh=mesh, in_specs=(split_rows, split_rows, P(), P(), P()),
        out_specs=(split_rows, split_rows), check_vma=False)
```

```python
import functools

import jax
import jax.numpy as jnp
from jax import lax
from jax.experimental import pallas as pl
from jax.experimental.pallas import tpu as pltpu
from jax.sharding import PartitionSpec as P

MESH = pl.DeviceIdType.MESH
BLK = 128
ROWS = 2
SLOTS = 8
UNIT = ROWS * BLK

OWN, NEAR, FAR, SIDE = 0, 1, 2, 3

RUN = 4
PARTS = 4
CHUNK = UNIT // PARTS
HALF = UNIT // 2

(Y_NO, Y_NN, Z_NO, Z_NN, T_NO, T_NN,
 Y_XO, Y_XX, Z_XO, Z_XX, T_XX,
 Y_SS, Z_SS, T_SS) = range(14)
SIDES = (Y_SS, Z_SS, T_SS)
FARS = (Y_XX, Z_XX, T_XX)


def split(value):
    high = value.astype(jnp.bfloat16)
    low = (value - high.astype(jnp.float32)).astype(jnp.bfloat16)
    return high, low


def kernel(row_count, col_count, pat_hbm, keep_hbm, y_hbm, z_hbm, yn_ref, zn_ref,
           pat_ref, keep_ref, y_ref, z_ref,
           own_y, own_z, own_t, recv, relay, bypass, cross, yh, yl, zh, zl, th, tl, rh, rl, acc_y, acc_z, acc_p,
           send_sem, recv_sem, far_send, far_recv, side_send, side_recv, relay_send, relay_recv,
           last_send, last_recv, bypass_sem, load_sem):
    loads = [
        pltpu.make_async_copy(source, target, load_sem.at[i])
        for i, (source, target) in enumerate((
            (pat_hbm, pat_ref), (keep_hbm, keep_ref), (y_hbm, y_ref), (z_hbm, z_ref)))
    ]
    for load in loads:
        load.start()
    row = lax.axis_index("row")
    col = lax.axis_index("col")
    odd = lax.rem(row, 2)
    near = (row + 1 - 2 * odd, col)
    far = (lax.rem(row + row_count - 1 + 2 * odd, row_count), col)
    side = (row, lax.rem(col + 1, col_count))
    back = (row, lax.rem(col + col_count - 1, col_count))
    place = lax.rem(col, RUN)
    head = place == 0
    first_col = col - place
    twin_col = lax.rem(col + RUN, col_count)
    twin = (row, twin_col)
    twin_far = (far[0], twin_col)
    twin_back = (row, lax.rem(twin_col + col_count - 1, col_count))

    barrier = pltpu.get_barrier_semaphore()
    others = [near, twin_far]
    others += [(row, lax.rem(col + d, col_count)) for d in range(1, col_count)]
    others += [(far[0], first_col + d) for d in range(RUN)]
    for other in others:
        pl.semaphore_signal(barrier, inc=1, device_id=other, device_id_type=MESH)
    loads[0].wait()
    loads[1].wait()

    def first(place):
        return (place[0] * col_count + place[1]) * ROWS

    starts = [first(place) for place in ((row, col), near, far, side)]
    labels = [pat_ref[0, starts[q // ROWS] + q % ROWS] for q in range(SLOTS)]

    def pick(wanted, keys, values):
        found = values[0]
        for key, value in zip(keys[1:], values[1:]):
            found = jnp.where(key == wanted, value, found)
        return found

    numbers = [jnp.int32(k) for k in range(SLOTS)]
    keys = [[pat_ref[k, starts[OWN] + s] for k in range(SLOTS)] for s in range(ROWS)]
    keep = [[jnp.float32(1)] + [keep_ref[k, starts[OWN] + s].astype(jnp.float32) for k in range(1, SLOTS)]
            for s in range(ROWS)]
    slot_of = [[pick(labels[q], keys[s], numbers) for q in range(SLOTS)] for s in range(ROWS)]
    place_of = [[pick(keys[s][k], labels, numbers) for k in range(SLOTS)] for s in range(ROWS)]
    kept = [[pick(labels[q], keys[s], keep[s]) for q in range(SLOTS)] for s in range(ROWS)]
    kept_far = []
    for s in range(ROWS):
        far_keys = [pat_ref[k, starts[FAR] + s] for k in range(SLOTS)]
        far_keep = [keep_ref[k, starts[FAR] + s].astype(jnp.float32) for k in range(SLOTS)]
        kept_far.append([pick(labels[e], far_keys, far_keep) for e in range(ROWS)])

    def same(value, number):
        return jnp.full((BLK, BLK), value, jnp.int32) == number

    def blk(s, e):
        return pl.ds(s * BLK, BLK), pl.ds(e * BLK, BLK)

    for load, source, whole, high, low in (
            (loads[2], y_ref, own_y, yh, yl), (loads[3], z_ref, own_z, zh, zl)):
        load.wait()
        for g in range(4):
            for s in range(ROWS):
                for e in range(ROWS):
                    slot = slot_of[s][g * ROWS + e]
                    value = source[s, :, pl.ds(0, BLK)]
                    for k in range(1, SLOTS):
                        value = jnp.where(same(slot, k), source[s, :, pl.ds(k * BLK, BLK)], value)
                    h, l = split(value)
                    where = (g, *blk(s, e))
                    whole[where] = value
                    high[where] = h
                    low[where] = l

    pl.semaphore_wait(barrier, len(others))

    copies = {}

    def send(source, unit, target):
        copy = pltpu.make_async_remote_copy(
            src_ref=source, dst_ref=recv.at[unit], send_sem=send_sem.at[unit],
            recv_sem=recv_sem.at[unit], device_id=target, device_id_type=MESH)
        copy.start()
        copies[unit] = copy

    def chunk(j):
        return pl.ds(j * CHUNK, CHUNK)

    def remote(source, target, send_to, recv_from, device):
        return pltpu.make_async_remote_copy(
            src_ref=source, dst_ref=target, send_sem=send_to, recv_sem=recv_from,
            device_id=device, device_id_type=MESH)

    def far_copy(source, n, j):
        return remote(source.at[chunk(j)], recv.at[FARS[n], chunk(j)], far_send.at[n, j], far_recv.at[n, j], far)

    def side_copy(source, n, j):
        return remote(source.at[chunk(j)], recv.at[SIDES[n], chunk(j)], side_send.at[n, j], side_recv.at[n, j], back)

    def twin_copy(source, n, j):
        return remote(source.at[chunk(j)], relay.at[n, chunk(j)], far_send.at[n, j], relay_recv.at[n, j], twin)

    def on_far(n, j):
        return remote(relay.at[n, chunk(j)], recv.at[FARS[n], chunk(j)], relay_send.at[n, j], far_recv.at[n, j], twin_far)

    def on_side(n, j):
        return remote(relay.at[n, chunk(j)], recv.at[SIDES[n], chunk(j)], side_send.at[n, j], side_recv.at[n, j], twin_back)

    def send_own(source, n):
        @pl.when(head)
        def _():
            for j in range(PARTS):
                twin_copy(source, n, j).start()

        @pl.when(jnp.logical_not(head))
        def _():
            for j in range(PARTS):
                far_copy(source, n, j).start()
            for j in range(PARTS):
                side_copy(source, n, j).start()

    def pass_on(n, chunks=range(PARTS)):
        @pl.when(head)
        def _():
            for j in chunks:
                twin_copy(own_y.at[OWN], n, j).wait_recv()
                on_far(n, j).start()
                on_side(n, j).start()

    def last_copy(j):
        return remote(own_z.at[FAR, chunk(j)], recv.at[Z_XO, chunk(j)], last_send.at[j], last_recv.at[j], far)

    def detour_copy(j):
        return remote(own_z.at[FAR, chunk(j)], bypass, last_send.at[j], bypass_sem.at[0], (row, col + j))

    def on_detour():
        return remote(bypass, recv.at[Z_XO, chunk(place)], bypass_sem.at[1], last_recv.at[place], (far[0], first_col))

    def send_last_direct():
        last_copy(0).start()

        @pl.when(jnp.logical_not(head))
        def _():
            for j in range(1, PARTS):
                last_copy(j).start()

    def send_last_detour():
        @pl.when(head)
        def _():
            for j in range(1, PARTS):
                detour_copy(j).start()

    def pass_detour():
        @pl.when(jnp.logical_not(head))
        def _():
            detour_copy(0).wait_recv()
            on_detour().start()

    send(own_y.at[FAR], Y_XO, far)
    send_last_detour()
    send_own(own_y.at[OWN], 0)
    send_own(own_z.at[OWN], 1)
    send(own_y.at[NEAR], Y_NO, near)
    send(own_y.at[OWN], Y_NN, near)
    send(own_z.at[NEAR], Z_NO, near)
    send(own_z.at[OWN], Z_NN, near)

    def arrive(unit):
        if unit in SIDES:
            for j in range(PARTS):
                side_copy(own_y.at[OWN], SIDES.index(unit), j).wait_recv()
        elif unit in FARS:
            for j in range(PARTS):
                far_copy(own_y.at[OWN], FARS.index(unit), j).wait_recv()
        else:
            copies[unit].wait_recv()
        h, l = split(recv[unit])
        rh[unit] = h
        rl[unit] = l

    def mul(a_high, a_low, b_high, b_low):
        dot = functools.partial(jnp.dot, preferred_element_type=jnp.float32)
        return dot(a_high, b_high) + (dot(a_high, b_low) + dot(a_low, b_high))

    Y = lambda g: (yh[g], yl[g])
    Z = lambda g: (zh[g], zl[g])
    T = lambda g: (th[g], tl[g])
    R = lambda u: (rh[u], rl[u])

    def factor_of(product, region, s, e):
        value = (-0.5 * kept[s][region * ROWS + e]) * product[s * BLK:(s + 1) * BLK, e * BLK:(e + 1) * BLK]
        if region == OWN and s == e:
            eye = lax.broadcasted_iota(jnp.int32, (BLK, BLK), 0) == lax.broadcasted_iota(jnp.int32, (BLK, BLK), 1)
            value = value + jnp.where(eye, jnp.float32(1.5), jnp.float32(0))
        return value

    def set_factor(region, product):
        for s in range(ROWS):
            for e in range(ROWS):
                value = factor_of(product, region, s, e)
                h, l = split(value)
                where = (region, *blk(s, e))
                th[where] = h
                tl[where] = l
                if region in (OWN, NEAR):
                    own_t[where] = value

    def parts(g):
        return [(g * ROWS + e, s, blk_of(s, e)) for s in range(ROWS) for e in range(ROWS)]

    def blk_of(s, e):
        return slice(s * BLK, (s + 1) * BLK), slice(e * BLK, (e + 1) * BLK)

    def put(acc, g, value):
        for q, s, where in parts(g):
            acc[q, s] = value[where]

    def add(acc, g, value):
        for q, s, where in parts(g):
            acc[q, s] += value[where]

    def get(acc, g):
        rows = [jnp.concatenate([acc[g * ROWS + e, s] for e in range(ROWS)], axis=1) for s in range(ROWS)]
        return jnp.concatenate(rows, axis=0)

    arrive(Y_NO)
    put(acc_z, OWN, mul(*Z(OWN), *Y(OWN)) + mul(*Z(NEAR), *R(Y_NO)))
    arrive(Y_NN)
    set_factor(NEAR, mul(*Z(OWN), *Y(NEAR)) + mul(*Z(NEAR), *R(Y_NN)))
    send(own_t.at[NEAR], T_NO, near)
    put(acc_p, FAR, mul(*Z(OWN), *Y(FAR)))
    put(acc_p, SIDE, mul(*Z(OWN), *Y(SIDE)))
    put(acc_y, NEAR, mul(*Y(OWN), *T(NEAR)))
    pass_detour()
    pass_on(0)
    arrive(Y_XO)
    set_factor(OWN, get(acc_z, OWN) + mul(*Z(FAR), *R(Y_XO)))
    send_own(own_t.at[OWN], 2)
    send(own_t.at[OWN], T_NN, near)
    send_last_direct()
    pass_on(1, range(0, 1))
    arrive(Z_NO)
    arrive(Z_NN)
    put(acc_y, OWN, mul(*Y(OWN), *T(OWN)))
    put(acc_z, OWN, mul(*T(OWN), *Z(OWN)) + mul(*T(NEAR), *R(Z_NO)))
    pass_on(1, range(1, 2))
    put(acc_z, NEAR, mul(*T(OWN), *Z(NEAR)) + mul(*T(NEAR), *R(Z_NN)))
    arrive(T_NO)
    add(acc_y, OWN, mul(*Y(NEAR), *R(T_NO)))
    pass_on(1, range(2, 3))
    arrive(T_NN)
    add(acc_y, NEAR, mul(*Y(NEAR), *R(T_NN)))
    put(acc_z, FAR, mul(*T(OWN), *Z(FAR)))
    put(acc_z, SIDE, mul(*T(OWN), *Z(SIDE)))
    pass_on(1, range(3, 4))
    arrive(Y_XX)
    set_factor(FAR, get(acc_p, FAR) + mul(*Z(FAR), *R(Y_XX)))
    put(acc_y, FAR, mul(*Y(OWN), *T(FAR)))
    pass_on(2, range(0, 1))
    arrive(Y_SS)
    set_factor(SIDE, get(acc_p, SIDE) + mul(*Z(SIDE), *R(Y_SS)))
    put(acc_y, SIDE, mul(*Y(OWN), *T(SIDE)))
    pass_on(2, range(1, PARTS))
    arrive(Z_XX)
    add(acc_z, FAR, mul(*T(FAR), *R(Z_XX)))
    arrive(Z_SS)
    add(acc_z, SIDE, mul(*T(SIDE), *R(Z_SS)))
    cross[...] = mul(*R(Z_XX), *R(Y_XO))
    arrive(T_SS)
    add(acc_y, SIDE, mul(*Y(SIDE), *R(T_SS)))
    arrive(T_XX)
    add(acc_y, FAR, mul(*Y(FAR), *R(T_XX)))
    for s in range(ROWS):
        for j in range(s * PARTS // ROWS, (s + 1) * PARTS // ROWS):
            last_copy(j).wait_recv()
        rows = pl.ds(s * HALF, HALF)
        high, low = split(recv[Z_XO, rows])
        add(acc_z, OWN, mul(th[FAR, :, rows], tl[FAR, :, rows], high, low))
        value = cross[rows] + mul(high, low, *Y(OWN))
        value = -0.5 * jnp.concatenate(
            [kept_far[s][e] * value[:, e * BLK:(e + 1) * BLK] for e in range(ROWS)], axis=1)
        high, low = split(value)
        add(acc_y, OWN, mul(yh[FAR, :, rows], yl[FAR, :, rows], high, low))

    def emit(result, out):
        for s in range(ROWS):
            for p in range(SLOTS):
                out[s, :, pl.ds(p * BLK, BLK)] = keep[s][p] * result[place_of[s][p], s]

    emit(acc_z, zn_ref)
    emit(acc_y, yn_ref)
    for copy in copies.values():
        copy.wait_send()
    for j in range(PARTS):
        last_copy(j).wait_send()
    for n in range(len(FARS)):
        for j in range(PARTS):
            far_copy(own_y.at[OWN], n, j).wait_send()
            side_copy(own_y.at[OWN], n, j).wait_send()

    @pl.when(head)
    def _():
        for n in range(len(FARS)):
            for j in range(PARTS):
                on_far(n, j).wait_send()

    @pl.when(jnp.logical_not(head))
    def _():
        on_detour().wait_send()


def write_out(y_ref, z_ref, y_hbm, z_hbm, sem):
    copies = []
    for source, target in ((y_ref, y_hbm), (z_ref, z_hbm)):
        for s in range(ROWS):
            for part in range(2):
                where = (s, pl.ds(part * (BLK // 2), BLK // 2))
                copies.append(pltpu.make_async_copy(source.at[where], target.at[where], sem.at[len(copies)]))
    for copy in copies:
        copy.start()
    for copy in copies:
        copy.wait()


def local(row_count, col_count, sqrt_iterate, inverse_iterate, pattern, keep_mask, row_order):
    del row_order
    whole = jax.ShapeDtypeStruct(sqrt_iterate.shape, jnp.float32)
    unit = (UNIT, UNIT)
    vmem = pl.BlockSpec(memory_space=pltpu.VMEM)
    f32 = lambda n: pltpu.VMEM((n, *unit), jnp.float32)
    b16 = lambda n: pltpu.VMEM((n, *unit), jnp.bfloat16)
    hbm = pl.BlockSpec(memory_space=pltpu.HBM)
    stay = lambda array: pltpu.with_memory_space_constraint(array, pltpu.HBM)
    dma = pltpu.SemaphoreType.DMA
    results = pl.pallas_call(
        functools.partial(kernel, row_count, col_count),
        out_shape=(whole, whole),
        in_specs=[hbm] * 4,
        out_specs=(vmem, vmem),
        scratch_shapes=[
            pltpu.SMEM(pattern.shape[::-1], jnp.int32), pltpu.SMEM(pattern.shape[::-1], jnp.int32),
            pltpu.VMEM(whole.shape, jnp.float32), pltpu.VMEM(whole.shape, jnp.float32),
            f32(4), f32(4), f32(2), f32(14), f32(3), pltpu.VMEM((CHUNK, UNIT), jnp.float32), pltpu.VMEM(unit, jnp.float32),
            b16(4), b16(4), b16(4), b16(4), b16(4), b16(4), b16(14), b16(14),
            pltpu.VMEM((SLOTS, ROWS, BLK, BLK), jnp.float32),
            pltpu.VMEM((SLOTS, ROWS, BLK, BLK), jnp.float32),
            pltpu.VMEM((SLOTS, ROWS, BLK, BLK), jnp.float32),
            dma((14,)), dma((14,)), *[dma((3, PARTS))] * 6, dma((PARTS,)), dma((PARTS,)), dma((2,)), dma((4,)),
        ],
        compiler_params=pltpu.CompilerParams(
            collective_id=0, has_side_effects=True, vmem_limit_bytes=54_000_000),
    )(*map(stay, (pattern.T, keep_mask.T, sqrt_iterate, inverse_iterate)))
    return pl.pallas_call(
        write_out,
        out_shape=(whole, whole),
        in_specs=[vmem, vmem],
        out_specs=(hbm, hbm),
        scratch_shapes=[dma((8,))],
        compiler_params=pltpu.CompilerParams(vmem_limit_bytes=4194304),
    )(*results)


def solution(mesh):
    split_rows = P(("row", "col"), None, None)
    body = functools.partial(local, mesh.shape["row"], mesh.shape["col"])
    return jax.shard_map(
        body, mesh=mesh, in_specs=(split_rows, split_rows, P(), P(), P()),
        out_specs=(split_rows, split_rows), check_vma=False)
```

```python
import functools

import jax
import jax.numpy as jnp
from jax import lax
from jax.experimental import pallas as pl
from jax.experimental.pallas import tpu as pltpu
from jax.sharding import PartitionSpec as P

MESH = pl.DeviceIdType.MESH
BLK = 128
ROWS = 2
SLOTS = 8
UNIT = ROWS * BLK

OWN, NEAR, FAR, SIDE = 0, 1, 2, 3

RUN = 4
PARTS = 4
CHUNK = UNIT // PARTS
HALF = UNIT // 2
CARRY = 40
assert UNIT - (PARTS - 1) * CARRY >= HALF

(Y_NO, Y_NN, Z_NO, Z_NN, T_NO, T_NN,
 Y_XO, Y_XX, Z_XO, Z_XX, T_XX,
 Y_SS, Z_SS, T_SS) = range(14)
SIDES = (Y_SS, Z_SS, T_SS)
FARS = (Y_XX, Z_XX, T_XX)


def split(value):
    high = value.astype(jnp.bfloat16)
    low = (value - high.astype(jnp.float32)).astype(jnp.bfloat16)
    return high, low


def kernel(row_count, col_count, pat_hbm, keep_hbm, y_hbm, z_hbm, yn_ref, zn_ref,
           pat_ref, keep_ref, y_ref, z_ref,
           own_y, own_z, own_t, recv, relay, bypass, cross, yh, yl, zh, zl, th, tl, rh, rl, acc_y, acc_z, acc_p,
           send_sem, recv_sem, far_send, far_recv, side_send, side_recv, relay_send, relay_recv,
           last_send, last_recv, bypass_sem, load_sem, ready):
    loads = [
        pltpu.make_async_copy(source, target, load_sem.at[i])
        for i, (source, target) in enumerate((
            (pat_hbm, pat_ref), (keep_hbm, keep_ref), (y_hbm, y_ref), (z_hbm, z_ref)))
    ]
    for load in loads:
        load.start()
    row = lax.axis_index("row")
    col = lax.axis_index("col")
    odd = lax.rem(row, 2)
    near = (row + 1 - 2 * odd, col)
    far = (lax.rem(row + row_count - 1 + 2 * odd, row_count), col)
    back = (row, lax.rem(col + col_count - 1, col_count))
    place = lax.rem(col, RUN)
    head = place == 0
    first_col = col - place
    twin_col = lax.rem(col + RUN, col_count)
    twin = (row, twin_col)
    twin_far = (far[0], twin_col)
    twin_back = (row, lax.rem(twin_col + col_count - 1, col_count))

    barrier = pltpu.get_barrier_semaphore()
    def enter(*targets):
        for target in targets:
            pl.semaphore_signal(barrier, inc=1, device_id=target, device_id_type=MESH)

    enter(far, near)

    @pl.when(head)
    def _():
        enter(twin, twin_far)
        for d in range(1, RUN):
            enter((row, col + d), (far[0], col + d))

    @pl.when(jnp.logical_and(place > 0, place < RUN - 1))
    def _():
        enter((row, col + 1))

    loads[0].wait()
    loads[1].wait()

    def first(place):
        return (place[0] * col_count + place[1]) * ROWS

    starts = [first(place) for place in ((row, col), near, far, (row, lax.rem(col + 1, col_count)))]
    labels = [pat_ref[0, starts[q // ROWS] + q % ROWS] for q in range(SLOTS)]

    def pick(wanted, keys, values):
        found = values[0]
        for key, value in zip(keys[1:], values[1:]):
            found = jnp.where(key == wanted, value, found)
        return found

    numbers = [jnp.int32(k) for k in range(SLOTS)]
    keys = [[pat_ref[k, starts[OWN] + s] for k in range(SLOTS)] for s in range(ROWS)]
    keep = [[jnp.float32(1)] + [keep_ref[k, starts[OWN] + s].astype(jnp.float32) for k in range(1, SLOTS)]
            for s in range(ROWS)]
    slot_of = [[pick(labels[q], keys[s], numbers) for q in range(SLOTS)] for s in range(ROWS)]
    place_of = [[pick(keys[s][k], labels, numbers) for k in range(SLOTS)] for s in range(ROWS)]
    kept = [[pick(labels[q], keys[s], keep[s]) for q in range(SLOTS)] for s in range(ROWS)]
    kept_far = []
    for s in range(ROWS):
        far_keys = [pat_ref[k, starts[FAR] + s] for k in range(SLOTS)]
        far_keep = [keep_ref[k, starts[FAR] + s].astype(jnp.float32) for k in range(SLOTS)]
        kept_far.append([pick(labels[e], far_keys, far_keep) for e in range(ROWS)])

    def same(value, number):
        return jnp.full((BLK, BLK), value, jnp.int32) == number

    def blk(s, e):
        return pl.ds(s * BLK, BLK), pl.ds(e * BLK, BLK)

    for load, source, whole, high, low in (
            (loads[2], y_ref, own_y, yh, yl), (loads[3], z_ref, own_z, zh, zl)):
        load.wait()
        for g in range(4):
            for s in range(ROWS):
                for e in range(ROWS):
                    slot = slot_of[s][g * ROWS + e]
                    value = source[s, :, pl.ds(0, BLK)]
                    for k in range(1, SLOTS):
                        value = jnp.where(same(slot, k), source[s, :, pl.ds(k * BLK, BLK)], value)
                    h, l = split(value)
                    where = (g, *blk(s, e))
                    whole[where] = value
                    high[where] = h
                    low[where] = l

    pl.semaphore_wait(barrier, jnp.where(place > 1, 5, 4))

    @pl.when(jnp.logical_not(head))
    def _():
        pl.semaphore_signal(ready, inc=1, device_id=(row, first_col), device_id_type=MESH)

    copies = {}

    def send(source, unit, target):
        copy = pltpu.make_async_remote_copy(
            src_ref=source, dst_ref=recv.at[unit], send_sem=send_sem.at[unit],
            recv_sem=recv_sem.at[unit], device_id=target, device_id_type=MESH)
        copy.start()
        copies[unit] = copy

    def chunk(j):
        return pl.ds(j * CHUNK, CHUNK)

    def remote(source, target, send_to, recv_from, device):
        return pltpu.make_async_remote_copy(
            src_ref=source, dst_ref=target, send_sem=send_to, recv_sem=recv_from,
            device_id=device, device_id_type=MESH)

    def far_copy(source, n, j):
        return remote(source.at[chunk(j)], recv.at[FARS[n], chunk(j)], far_send.at[n, j], far_recv.at[n, j], far)

    def side_copy(source, n, j):
        return remote(source.at[chunk(j)], recv.at[SIDES[n], chunk(j)], side_send.at[n, j], side_recv.at[n, j], back)

    def twin_copy(source, n, j):
        return remote(source.at[chunk(j)], relay.at[n, chunk(j)], far_send.at[n, j], relay_recv.at[n, j], twin)

    def on_far(n, j):
        return remote(relay.at[n, chunk(j)], recv.at[FARS[n], chunk(j)], relay_send.at[n, j], far_recv.at[n, j], twin_far)

    def on_side(n, j):
        return remote(relay.at[n, chunk(j)], recv.at[SIDES[n], chunk(j)], side_send.at[n, j], side_recv.at[n, j], twin_back)

    def send_own(source, n):
        @pl.when(head)
        def _():
            for j in range(PARTS):
                twin_copy(source, n, j).start()

        @pl.when(jnp.logical_not(head))
        def _():
            for j in range(PARTS):
                far_copy(source, n, j).start()
            for j in range(PARTS):
                side_copy(source, n, j).start()

    def pass_on(n, chunks=range(PARTS)):
        @pl.when(head)
        def _():
            for j in chunks:
                twin_copy(own_y.at[OWN], n, j).wait_recv()
                on_far(n, j).start()
                on_side(n, j).start()

    def carried(j):
        return pl.ds(pl.multiple_of(UNIT - (PARTS - j) * CARRY, 8), CARRY)

    def last_rows(j):
        return carried(j) if j else pl.ds(0, UNIT - (PARTS - 1) * CARRY)

    def last_copy(j):
        return remote(own_z.at[FAR, last_rows(j)], recv.at[Z_XO, last_rows(j)], last_send.at[j], last_recv.at[j], far)

    def detour_copy(j):
        return remote(own_z.at[FAR, carried(j)], bypass, last_send.at[j], bypass_sem.at[0], (row, col + j))

    def on_detour():
        return remote(bypass, recv.at[Z_XO, carried(place)], bypass_sem.at[1], last_recv.at[place], (far[0], first_col))

    def send_last_direct():
        @pl.when(jnp.logical_not(head))
        def _():
            for j in range(PARTS):
                last_copy(j).start()

    def send_last_detour():
        @pl.when(head)
        def _():
            pl.semaphore_wait(ready, RUN - 1)
            for j in range(1, PARTS):
                detour_copy(j).start()

    def pass_detour():
        @pl.when(jnp.logical_not(head))
        def _():
            detour_copy(1).wait_recv()
            on_detour().start()

    send(own_y.at[FAR], Y_XO, far)
    send_own(own_y.at[OWN], 0)
    send_own(own_z.at[OWN], 1)
    send(own_y.at[NEAR], Y_NO, near)
    send(own_y.at[OWN], Y_NN, near)
    send(own_z.at[NEAR], Z_NO, near)
    send(own_z.at[OWN], Z_NN, near)

    def arrive(unit):
        if unit in SIDES:
            for j in range(PARTS):
                side_copy(own_y.at[OWN], SIDES.index(unit), j).wait_recv()
        elif unit in FARS:
            for j in range(PARTS):
                far_copy(own_y.at[OWN], FARS.index(unit), j).wait_recv()
        else:
            copies[unit].wait_recv()
        h, l = split(recv[unit])
        rh[unit] = h
        rl[unit] = l

    def mul(a_high, a_low, b_high, b_low):
        dot = functools.partial(jnp.dot, preferred_element_type=jnp.float32)
        return dot(a_high, b_high) + (dot(a_high, b_low) + dot(a_low, b_high))

    Y = lambda g: (yh[g], yl[g])
    Z = lambda g: (zh[g], zl[g])
    T = lambda g: (th[g], tl[g])
    R = lambda u: (rh[u], rl[u])

    def factor_of(product, region, s, e):
        value = (-0.5 * kept[s][region * ROWS + e]) * product[s * BLK:(s + 1) * BLK, e * BLK:(e + 1) * BLK]
        if region == OWN and s == e:
            eye = lax.broadcasted_iota(jnp.int32, (BLK, BLK), 0) == lax.broadcasted_iota(jnp.int32, (BLK, BLK), 1)
            value = value + jnp.where(eye, jnp.float32(1.5), jnp.float32(0))
        return value

    def set_factor(region, product):
        for s in range(ROWS):
            for e in range(ROWS):
                value = factor_of(product, region, s, e)
                h, l = split(value)
                where = (region, *blk(s, e))
                th[where] = h
                tl[where] = l
                if region in (OWN, NEAR):
                    own_t[where] = value

    def parts(g):
        return [(g * ROWS + e, s, blk_of(s, e)) for s in range(ROWS) for e in range(ROWS)]

    def blk_of(s, e):
        return slice(s * BLK, (s + 1) * BLK), slice(e * BLK, (e + 1) * BLK)

    def put(acc, g, value):
        for q, s, where in parts(g):
            acc[q, s] = value[where]

    def add(acc, g, value):
        for q, s, where in parts(g):
            acc[q, s] += value[where]

    def get(acc, g):
        rows = [jnp.concatenate([acc[g * ROWS + e, s] for e in range(ROWS)], axis=1) for s in range(ROWS)]
        return jnp.concatenate(rows, axis=0)

    arrive(Y_NO)
    put(acc_z, OWN, mul(*Z(OWN), *Y(OWN)) + mul(*Z(NEAR), *R(Y_NO)))
    arrive(Y_NN)
    set_factor(NEAR, mul(*Z(OWN), *Y(NEAR)) + mul(*Z(NEAR), *R(Y_NN)))
    send(own_t.at[NEAR], T_NO, near)
    put(acc_p, FAR, mul(*Z(OWN), *Y(FAR)))
    put(acc_p, SIDE, mul(*Z(OWN), *Y(SIDE)))
    put(acc_y, NEAR, mul(*Y(OWN), *T(NEAR)))
    send_last_detour()
    pass_detour()
    pass_on(0)
    arrive(Y_XO)
    set_factor(OWN, get(acc_z, OWN) + mul(*Z(FAR), *R(Y_XO)))
    @pl.when(head)
    def _():
        last_copy(0).start()

    send_own(own_t.at[OWN], 2)
    send(own_t.at[OWN], T_NN, near)
    send_last_direct()
    pass_on(1, range(0, 1))
    arrive(Z_NO)
    arrive(Z_NN)
    put(acc_y, OWN, mul(*Y(OWN), *T(OWN)))
    put(acc_z, OWN, mul(*T(OWN), *Z(OWN)) + mul(*T(NEAR), *R(Z_NO)))
    pass_on(1, range(1, 2))
    put(acc_z, NEAR, mul(*T(OWN), *Z(NEAR)) + mul(*T(NEAR), *R(Z_NN)))
    arrive(T_NO)
    add(acc_y, OWN, mul(*Y(NEAR), *R(T_NO)))
    pass_on(1, range(2, 3))
    arrive(T_NN)
    add(acc_y, NEAR, mul(*Y(NEAR), *R(T_NN)))
    put(acc_z, FAR, mul(*T(OWN), *Z(FAR)))
    put(acc_z, SIDE, mul(*T(OWN), *Z(SIDE)))
    pass_on(1, range(3, 4))
    arrive(Y_XX)
    set_factor(FAR, get(acc_p, FAR) + mul(*Z(FAR), *R(Y_XX)))
    put(acc_y, FAR, mul(*Y(OWN), *T(FAR)))
    pass_on(2, range(0, 1))
    arrive(Y_SS)
    set_factor(SIDE, get(acc_p, SIDE) + mul(*Z(SIDE), *R(Y_SS)))
    put(acc_y, SIDE, mul(*Y(OWN), *T(SIDE)))
    pass_on(2, range(1, PARTS))
    arrive(Z_XX)
    add(acc_z, FAR, mul(*T(FAR), *R(Z_XX)))
    arrive(Z_SS)
    add(acc_z, SIDE, mul(*T(SIDE), *R(Z_SS)))
    cross[...] = mul(*R(Z_XX), *R(Y_XO))
    arrive(T_SS)
    add(acc_y, SIDE, mul(*Y(SIDE), *R(T_SS)))
    arrive(T_XX)
    add(acc_y, FAR, mul(*Y(FAR), *R(T_XX)))
    for s in range(ROWS):
        for j in ((0,), range(1, PARTS))[s]:
            last_copy(j).wait_recv()
        rows = pl.ds(s * HALF, HALF)
        high, low = split(recv[Z_XO, rows])
        add(acc_z, OWN, mul(th[FAR, :, rows], tl[FAR, :, rows], high, low))
        value = cross[rows] + mul(high, low, *Y(OWN))
        value = -0.5 * jnp.concatenate(
            [kept_far[s][e] * value[:, e * BLK:(e + 1) * BLK] for e in range(ROWS)], axis=1)
        high, low = split(value)
        add(acc_y, OWN, mul(yh[FAR, :, rows], yl[FAR, :, rows], high, low))

    def emit(result, out):
        for s in range(ROWS):
            for p in range(SLOTS):
                out[s, :, pl.ds(p * BLK, BLK)] = keep[s][p] * result[place_of[s][p], s]

    emit(acc_z, zn_ref)
    emit(acc_y, yn_ref)
    for copy in copies.values():
        copy.wait_send()
    for j in range(PARTS):
        last_copy(j).wait_send()
    for n in range(len(FARS)):
        for j in range(PARTS):
            far_copy(own_y.at[OWN], n, j).wait_send()
            side_copy(own_y.at[OWN], n, j).wait_send()

    @pl.when(head)
    def _():
        for n in range(len(FARS)):
            for j in range(PARTS):
                on_far(n, j).wait_send()

    @pl.when(jnp.logical_not(head))
    def _():
        on_detour().wait_send()


def write_out(y_ref, z_ref, y_hbm, z_hbm, sem):
    copies = []
    for source, target in ((y_ref, y_hbm), (z_ref, z_hbm)):
        for s in range(ROWS):
            for part in range(2):
                where = (s, pl.ds(part * (BLK // 2), BLK // 2))
                copies.append(pltpu.make_async_copy(source.at[where], target.at[where], sem.at[len(copies)]))
    for copy in copies:
        copy.start()
    for copy in copies:
        copy.wait()


def local(row_count, col_count, sqrt_iterate, inverse_iterate, pattern, keep_mask, row_order):
    del row_order
    whole = jax.ShapeDtypeStruct(sqrt_iterate.shape, jnp.float32)
    unit = (UNIT, UNIT)
    vmem = pl.BlockSpec(memory_space=pltpu.VMEM)
    f32 = lambda n: pltpu.VMEM((n, *unit), jnp.float32)
    b16 = lambda n: pltpu.VMEM((n, *unit), jnp.bfloat16)
    hbm = pl.BlockSpec(memory_space=pltpu.HBM)
    stay = lambda array: pltpu.with_memory_space_constraint(array, pltpu.HBM)
    dma = pltpu.SemaphoreType.DMA
    results = pl.pallas_call(
        functools.partial(kernel, row_count, col_count),
        out_shape=(whole, whole),
        in_specs=[hbm] * 4,
        out_specs=(vmem, vmem),
        scratch_shapes=[
            pltpu.SMEM(pattern.shape[::-1], jnp.int32), pltpu.SMEM(pattern.shape[::-1], jnp.int32),
            pltpu.VMEM(whole.shape, jnp.float32), pltpu.VMEM(whole.shape, jnp.float32),
            f32(4), f32(4), f32(2), f32(14), f32(3), pltpu.VMEM((CARRY, UNIT), jnp.float32), pltpu.VMEM(unit, jnp.float32),
            b16(4), b16(4), b16(4), b16(4), b16(4), b16(4), b16(14), b16(14),
            pltpu.VMEM((SLOTS, ROWS, BLK, BLK), jnp.float32),
            pltpu.VMEM((SLOTS, ROWS, BLK, BLK), jnp.float32),
            pltpu.VMEM((SLOTS, ROWS, BLK, BLK), jnp.float32),
            dma((14,)), dma((14,)), *[dma((3, PARTS))] * 6, dma((PARTS,)), dma((PARTS,)), dma((2,)), dma((4,)), pltpu.SemaphoreType.REGULAR,
        ],
        compiler_params=pltpu.CompilerParams(
            collective_id=0, has_side_effects=True, vmem_limit_bytes=54_000_000),
    )(*map(stay, (pattern.T, keep_mask.T, sqrt_iterate, inverse_iterate)))
    return pl.pallas_call(
        write_out,
        out_shape=(whole, whole),
        in_specs=[vmem, vmem],
        out_specs=(hbm, hbm),
        scratch_shapes=[dma((8,))],
        compiler_params=pltpu.CompilerParams(vmem_limit_bytes=4194304),
    )(*results)


def solution(mesh):
    split_rows = P(("row", "col"), None, None)
    body = functools.partial(local, mesh.shape["row"], mesh.shape["col"])
    return jax.shard_map(
        body, mesh=mesh, in_specs=(split_rows, split_rows, P(), P(), P()),
        out_specs=(split_rows, split_rows), check_vma=False)
```

```python
import functools

import jax
import jax.numpy as jnp
from jax import lax
from jax.experimental import pallas as pl
from jax.experimental.pallas import tpu as pltpu
from jax.sharding import PartitionSpec as P

MESH = pl.DeviceIdType.MESH
BLK = 128
ROWS = 2
SLOTS = 8
UNIT = ROWS * BLK

OWN, NEAR, FAR, SIDE = 0, 1, 2, 3

RUN = 4
PARTS = 4
CHUNK = UNIT // PARTS
HALF = UNIT // 2
CARRY = 40
assert UNIT - (PARTS - 1) * CARRY >= HALF

(Y_NO, Y_NN, Z_NO, Z_NN, T_NO, T_NN,
 Y_XO, Y_XX, Z_XO, Z_XX, T_XX,
 Y_SS, Z_SS, T_SS) = range(14)
SIDES = (Y_SS, Z_SS, T_SS)
FARS = (Y_XX, Z_XX, T_XX)


def split(value):
    high = value.astype(jnp.bfloat16)
    low = (value - high.astype(jnp.float32)).astype(jnp.bfloat16)
    return high, low


def kernel(row_count, col_count, pat_hbm, keep_hbm, y_hbm, z_hbm, yn_ref, zn_ref,
           pat_ref, keep_ref, y_ref, z_ref,
           own_y, own_z, own_t, recv, relay, bypass, cross, yh, yl, zh, zl, th, tl, rh, rl, acc_y, acc_z, acc_p,
           send_sem, recv_sem, far_send, far_recv, side_send, side_recv, relay_send, relay_recv,
           last_send, last_recv, bypass_sem, load_sem, ready):
    loads = [
        pltpu.make_async_copy(source, target, load_sem.at[i])
        for i, (source, target) in enumerate((
            (pat_hbm, pat_ref), (keep_hbm, keep_ref), (y_hbm, y_ref), (z_hbm, z_ref)))
    ]
    for load in loads:
        load.start()
    row = lax.axis_index("row")
    col = lax.axis_index("col")
    odd = lax.rem(row, 2)
    near = (row + 1 - 2 * odd, col)
    far = (lax.rem(row + row_count - 1 + 2 * odd, row_count), col)
    back = (row, lax.rem(col + col_count - 1, col_count))
    place = lax.rem(col, RUN)
    head = place == 0
    first_col = col - place
    twin_col = lax.rem(col + RUN, col_count)
    twin = (row, twin_col)
    twin_far = (far[0], twin_col)
    twin_back = (row, lax.rem(twin_col + col_count - 1, col_count))

    barrier = pltpu.get_barrier_semaphore()
    def enter(*targets):
        for target in targets:
            pl.semaphore_signal(barrier, inc=1, device_id=target, device_id_type=MESH)

    enter(far, near)

    @pl.when(head)
    def _():
        enter(twin, twin_far)
        for d in range(1, RUN):
            enter((row, col + d), (far[0], col + d))

    @pl.when(jnp.logical_and(place > 0, place < RUN - 1))
    def _():
        enter((row, col + 1))

    loads[0].wait()
    loads[1].wait()

    def first(place):
        return (place[0] * col_count + place[1]) * ROWS

    starts = [first(place) for place in ((row, col), near, far, (row, lax.rem(col + 1, col_count)))]
    labels = [pat_ref[0, starts[q // ROWS] + q % ROWS] for q in range(SLOTS)]

    def pick(wanted, keys, values):
        found = values[0]
        for key, value in zip(keys[1:], values[1:]):
            found = jnp.where(key == wanted, value, found)
        return found

    numbers = [jnp.int32(k) for k in range(SLOTS)]
    keys = [[pat_ref[k, starts[OWN] + s] for k in range(SLOTS)] for s in range(ROWS)]
    keep = [[jnp.float32(1)] + [keep_ref[k, starts[OWN] + s].astype(jnp.float32) for k in range(1, SLOTS)]
            for s in range(ROWS)]
    slot_of = [[pick(labels[q], keys[s], numbers) for q in range(SLOTS)] for s in range(ROWS)]
    place_of = [[pick(keys[s][k], labels, numbers) for k in range(SLOTS)] for s in range(ROWS)]
    kept = [[pick(labels[q], keys[s], keep[s]) for q in range(SLOTS)] for s in range(ROWS)]
    kept_far = []
    for s in range(ROWS):
        far_keys = [pat_ref[k, starts[FAR] + s] for k in range(SLOTS)]
        far_keep = [keep_ref[k, starts[FAR] + s].astype(jnp.float32) for k in range(SLOTS)]
        kept_far.append([pick(labels[e], far_keys, far_keep) for e in range(ROWS)])

    def same(value, number):
        return jnp.full((BLK, BLK), value, jnp.int32) == number

    def blk(s, e):
        return pl.ds(s * BLK, BLK), pl.ds(e * BLK, BLK)

    def arrange(load, source, whole, high, low):
        load.wait()
        for g in (FAR, OWN, NEAR, SIDE):
            for s in range(ROWS):
                for e in range(ROWS):
                    slot = slot_of[s][g * ROWS + e]
                    value = source[s, :, pl.ds(0, BLK)]
                    for k in range(1, SLOTS):
                        value = jnp.where(same(slot, k), source[s, :, pl.ds(k * BLK, BLK)], value)
                    h, l = split(value)
                    where = (g, *blk(s, e))
                    whole[where] = value
                    high[where] = h
                    low[where] = l

    arrange(loads[2], y_ref, own_y, yh, yl)
    pl.semaphore_wait(barrier, jnp.where(place > 1, 5, 4))

    @pl.when(jnp.logical_not(head))
    def _():
        pl.semaphore_signal(ready, inc=1, device_id=(row, first_col), device_id_type=MESH)

    copies = {}

    def send(source, unit, target):
        copy = pltpu.make_async_remote_copy(
            src_ref=source, dst_ref=recv.at[unit], send_sem=send_sem.at[unit],
            recv_sem=recv_sem.at[unit], device_id=target, device_id_type=MESH)
        copy.start()
        copies[unit] = copy

    def chunk(j):
        return pl.ds(j * CHUNK, CHUNK)

    def remote(source, target, send_to, recv_from, device):
        return pltpu.make_async_remote_copy(
            src_ref=source, dst_ref=target, send_sem=send_to, recv_sem=recv_from,
            device_id=device, device_id_type=MESH)

    def far_copy(source, n, j):
        return remote(source.at[chunk(j)], recv.at[FARS[n], chunk(j)], far_send.at[n, j], far_recv.at[n, j], far)

    def side_copy(source, n, j):
        return remote(source.at[chunk(j)], recv.at[SIDES[n], chunk(j)], side_send.at[n, j], side_recv.at[n, j], back)

    def twin_copy(source, n, j):
        return remote(source.at[chunk(j)], relay.at[n, chunk(j)], far_send.at[n, j], relay_recv.at[n, j], twin)

    def on_far(n, j):
        return remote(relay.at[n, chunk(j)], recv.at[FARS[n], chunk(j)], relay_send.at[n, j], far_recv.at[n, j], twin_far)

    def on_side(n, j):
        return remote(relay.at[n, chunk(j)], recv.at[SIDES[n], chunk(j)], side_send.at[n, j], side_recv.at[n, j], twin_back)

    def send_own(source, n):
        @pl.when(head)
        def _():
            for j in range(PARTS):
                twin_copy(source, n, j).start()

        @pl.when(jnp.logical_not(head))
        def _():
            for j in range(PARTS):
                far_copy(source, n, j).start()
            for j in range(PARTS):
                side_copy(source, n, j).start()

    def pass_on(n, chunks=range(PARTS)):
        @pl.when(head)
        def _():
            for j in chunks:
                twin_copy(own_y.at[OWN], n, j).wait_recv()
                on_far(n, j).start()
                on_side(n, j).start()

    def carried(j):
        return pl.ds(pl.multiple_of(UNIT - (PARTS - j) * CARRY, 8), CARRY)

    def last_rows(j):
        return carried(j) if j else pl.ds(0, UNIT - (PARTS - 1) * CARRY)

    def last_copy(j):
        return remote(own_z.at[FAR, last_rows(j)], recv.at[Z_XO, last_rows(j)], last_send.at[j], last_recv.at[j], far)

    def detour_copy(j):
        return remote(own_z.at[FAR, carried(j)], bypass, last_send.at[j], bypass_sem.at[0], (row, col + j))

    def on_detour():
        return remote(bypass, recv.at[Z_XO, carried(place)], bypass_sem.at[1], last_recv.at[place], (far[0], first_col))

    def send_last_direct():
        @pl.when(jnp.logical_not(head))
        def _():
            for j in range(PARTS):
                last_copy(j).start()

    def send_last_detour():
        @pl.when(head)
        def _():
            pl.semaphore_wait(ready, RUN - 1)
            for j in range(1, PARTS):
                detour_copy(j).start()

    def pass_detour():
        @pl.when(jnp.logical_not(head))
        def _():
            detour_copy(1).wait_recv()
            on_detour().start()

    send(own_y.at[FAR], Y_XO, far)
    send_own(own_y.at[OWN], 0)
    send(own_y.at[NEAR], Y_NO, near)
    send(own_y.at[OWN], Y_NN, near)
    arrange(loads[3], z_ref, own_z, zh, zl)
    send_own(own_z.at[OWN], 1)
    send(own_z.at[NEAR], Z_NO, near)
    send(own_z.at[OWN], Z_NN, near)

    def arrive(unit):
        if unit in SIDES:
            for j in range(PARTS):
                side_copy(own_y.at[OWN], SIDES.index(unit), j).wait_recv()
        elif unit in FARS:
            for j in range(PARTS):
                far_copy(own_y.at[OWN], FARS.index(unit), j).wait_recv()
        else:
            copies[unit].wait_recv()
        h, l = split(recv[unit])
        rh[unit] = h
        rl[unit] = l

    def mul(a_high, a_low, b_high, b_low):
        dot = functools.partial(jnp.dot, preferred_element_type=jnp.float32)
        return dot(a_high, b_high) + (dot(a_high, b_low) + dot(a_low, b_high))

    Y = lambda g: (yh[g], yl[g])
    Z = lambda g: (zh[g], zl[g])
    T = lambda g: (th[g], tl[g])
    R = lambda u: (rh[u], rl[u])

    def factor_of(product, region, s, e):
        value = (-0.5 * kept[s][region * ROWS + e]) * product[s * BLK:(s + 1) * BLK, e * BLK:(e + 1) * BLK]
        if region == OWN and s == e:
            eye = lax.broadcasted_iota(jnp.int32, (BLK, BLK), 0) == lax.broadcasted_iota(jnp.int32, (BLK, BLK), 1)
            value = value + jnp.where(eye, jnp.float32(1.5), jnp.float32(0))
        return value

    def set_factor(region, product):
        for s in range(ROWS):
            for e in range(ROWS):
                value = factor_of(product, region, s, e)
                h, l = split(value)
                where = (region, *blk(s, e))
                th[where] = h
                tl[where] = l
                if region in (OWN, NEAR):
                    own_t[where] = value

    def parts(g):
        return [(g * ROWS + e, s, blk_of(s, e)) for s in range(ROWS) for e in range(ROWS)]

    def blk_of(s, e):
        return slice(s * BLK, (s + 1) * BLK), slice(e * BLK, (e + 1) * BLK)

    def put(acc, g, value):
        for q, s, where in parts(g):
            acc[q, s] = value[where]

    def add(acc, g, value):
        for q, s, where in parts(g):
            acc[q, s] += value[where]

    def get(acc, g):
        rows = [jnp.concatenate([acc[g * ROWS + e, s] for e in range(ROWS)], axis=1) for s in range(ROWS)]
        return jnp.concatenate(rows, axis=0)

    arrive(Y_NO)
    put(acc_z, OWN, mul(*Z(OWN), *Y(OWN)) + mul(*Z(NEAR), *R(Y_NO)))
    arrive(Y_NN)
    set_factor(NEAR, mul(*Z(OWN), *Y(NEAR)) + mul(*Z(NEAR), *R(Y_NN)))
    send(own_t.at[NEAR], T_NO, near)
    put(acc_p, FAR, mul(*Z(OWN), *Y(FAR)))
    put(acc_p, SIDE, mul(*Z(OWN), *Y(SIDE)))
    put(acc_y, NEAR, mul(*Y(OWN), *T(NEAR)))
    send_last_detour()
    pass_detour()
    pass_on(0)
    arrive(Y_XO)
    set_factor(OWN, get(acc_z, OWN) + mul(*Z(FAR), *R(Y_XO)))
    @pl.when(head)
    def _():
        last_copy(0).start()

    send_own(own_t.at[OWN], 2)
    send(own_t.at[OWN], T_NN, near)
    send_last_direct()
    pass_on(1, range(0, 1))
    arrive(Z_NO)
    arrive(Z_NN)
    put(acc_y, OWN, mul(*Y(OWN), *T(OWN)))
    put(acc_z, OWN, mul(*T(OWN), *Z(OWN)) + mul(*T(NEAR), *R(Z_NO)))
    pass_on(1, range(1, 2))
    put(acc_z, NEAR, mul(*T(OWN), *Z(NEAR)) + mul(*T(NEAR), *R(Z_NN)))
    arrive(T_NO)
    add(acc_y, OWN, mul(*Y(NEAR), *R(T_NO)))
    pass_on(1, range(2, 3))
    arrive(T_NN)
    add(acc_y, NEAR, mul(*Y(NEAR), *R(T_NN)))
    put(acc_z, FAR, mul(*T(OWN), *Z(FAR)))
    put(acc_z, SIDE, mul(*T(OWN), *Z(SIDE)))
    pass_on(1, range(3, 4))
    arrive(Y_XX)
    set_factor(FAR, get(acc_p, FAR) + mul(*Z(FAR), *R(Y_XX)))
    put(acc_y, FAR, mul(*Y(OWN), *T(FAR)))
    pass_on(2, range(0, 1))
    arrive(Y_SS)
    set_factor(SIDE, get(acc_p, SIDE) + mul(*Z(SIDE), *R(Y_SS)))
    put(acc_y, SIDE, mul(*Y(OWN), *T(SIDE)))
    pass_on(2, range(1, PARTS))
    arrive(Z_XX)
    add(acc_z, FAR, mul(*T(FAR), *R(Z_XX)))
    arrive(Z_SS)
    add(acc_z, SIDE, mul(*T(SIDE), *R(Z_SS)))
    cross[...] = mul(*R(Z_XX), *R(Y_XO))
    arrive(T_SS)
    add(acc_y, SIDE, mul(*Y(SIDE), *R(T_SS)))
    arrive(T_XX)
    add(acc_y, FAR, mul(*Y(FAR), *R(T_XX)))
    for s in range(ROWS):
        for j in ((0,), range(1, PARTS))[s]:
            last_copy(j).wait_recv()
        rows = pl.ds(s * HALF, HALF)
        high, low = split(recv[Z_XO, rows])
        add(acc_z, OWN, mul(th[FAR, :, rows], tl[FAR, :, rows], high, low))
        value = cross[rows] + mul(high, low, *Y(OWN))
        value = -0.5 * jnp.concatenate(
            [kept_far[s][e] * value[:, e * BLK:(e + 1) * BLK] for e in range(ROWS)], axis=1)
        high, low = split(value)
        add(acc_y, OWN, mul(yh[FAR, :, rows], yl[FAR, :, rows], high, low))

    def emit(result, out):
        for s in range(ROWS):
            for p in range(SLOTS):
                out[s, :, pl.ds(p * BLK, BLK)] = keep[s][p] * result[place_of[s][p], s]

    emit(acc_z, zn_ref)
    emit(acc_y, yn_ref)
    for copy in copies.values():
        copy.wait_send()
    for j in range(PARTS):
        last_copy(j).wait_send()
    for n in range(len(FARS)):
        for j in range(PARTS):
            far_copy(own_y.at[OWN], n, j).wait_send()
            side_copy(own_y.at[OWN], n, j).wait_send()

    @pl.when(head)
    def _():
        for n in range(len(FARS)):
            for j in range(PARTS):
                on_far(n, j).wait_send()

    @pl.when(jnp.logical_not(head))
    def _():
        on_detour().wait_send()


def write_out(y_ref, z_ref, y_hbm, z_hbm, sem):
    copies = []
    for source, target in ((y_ref, y_hbm), (z_ref, z_hbm)):
        for s in range(ROWS):
            for part in range(2):
                where = (s, pl.ds(part * (BLK // 2), BLK // 2))
                copies.append(pltpu.make_async_copy(source.at[where], target.at[where], sem.at[len(copies)]))
    for copy in copies:
        copy.start()
    for copy in copies:
        copy.wait()


def local(row_count, col_count, sqrt_iterate, inverse_iterate, pattern, keep_mask, row_order):
    del row_order
    whole = jax.ShapeDtypeStruct(sqrt_iterate.shape, jnp.float32)
    unit = (UNIT, UNIT)
    vmem = pl.BlockSpec(memory_space=pltpu.VMEM)
    f32 = lambda n: pltpu.VMEM((n, *unit), jnp.float32)
    b16 = lambda n: pltpu.VMEM((n, *unit), jnp.bfloat16)
    hbm = pl.BlockSpec(memory_space=pltpu.HBM)
    stay = lambda array: pltpu.with_memory_space_constraint(array, pltpu.HBM)
    dma = pltpu.SemaphoreType.DMA
    results = pl.pallas_call(
        functools.partial(kernel, row_count, col_count),
        out_shape=(whole, whole),
        in_specs=[hbm] * 4,
        out_specs=(vmem, vmem),
        scratch_shapes=[
            pltpu.SMEM(pattern.shape[::-1], jnp.int32), pltpu.SMEM(pattern.shape[::-1], jnp.int32),
            pltpu.VMEM(whole.shape, jnp.float32), pltpu.VMEM(whole.shape, jnp.float32),
            f32(4), f32(4), f32(2), f32(14), f32(3), pltpu.VMEM((CARRY, UNIT), jnp.float32), pltpu.VMEM(unit, jnp.float32),
            b16(4), b16(4), b16(4), b16(4), b16(4), b16(4), b16(14), b16(14),
            pltpu.VMEM((SLOTS, ROWS, BLK, BLK), jnp.float32),
            pltpu.VMEM((SLOTS, ROWS, BLK, BLK), jnp.float32),
            pltpu.VMEM((SLOTS, ROWS, BLK, BLK), jnp.float32),
            dma((14,)), dma((14,)), *[dma((3, PARTS))] * 6, dma((PARTS,)), dma((PARTS,)), dma((2,)), dma((4,)), pltpu.SemaphoreType.REGULAR,
        ],
        compiler_params=pltpu.CompilerParams(
            collective_id=0, has_side_effects=True, vmem_limit_bytes=54_000_000),
    )(*map(stay, (pattern.T, keep_mask.T, sqrt_iterate, inverse_iterate)))
    return pl.pallas_call(
        write_out,
        out_shape=(whole, whole),
        in_specs=[vmem, vmem],
        out_specs=(hbm, hbm),
        scratch_shapes=[dma((8,))],
        compiler_params=pltpu.CompilerParams(vmem_limit_bytes=4194304),
    )(*results)


def solution(mesh):
    split_rows = P(("row", "col"), None, None)
    body = functools.partial(local, mesh.shape["row"], mesh.shape["col"])
    return jax.shard_map(
        body, mesh=mesh, in_specs=(split_rows, split_rows, P(), P(), P()),
        out_specs=(split_rows, split_rows), check_vma=False)
```

```python
import functools

import jax
import jax.numpy as jnp
from jax import lax
from jax.experimental import pallas as pl
from jax.experimental.pallas import tpu as pltpu
from jax.sharding import PartitionSpec as P

MESH = pl.DeviceIdType.MESH
BLK = 128
ROWS = 2
SLOTS = 8
UNIT = ROWS * BLK

OWN, NEAR, FAR, SIDE = 0, 1, 2, 3

RUN = 4
PARTS = 4
CHUNK = UNIT // PARTS
HALF = UNIT // 2
CARRY = 40
assert UNIT - (RUN - 1) * CARRY >= HALF

(Y_NO, Y_NN, Z_NO, Z_NN, T_NO, T_NN,
 Y_XO, Y_XX, Z_XO, Z_XX, T_XX,
 Y_SS, Z_SS, T_SS) = range(14)
SIDES = (Y_SS, Z_SS, T_SS)
FARS = (Y_XX, Z_XX, T_XX)


def split(value):
    high = value.astype(jnp.bfloat16)
    low = (value - high.astype(jnp.float32)).astype(jnp.bfloat16)
    return high, low


def kernel(row_count, col_count, pat_hbm, keep_hbm, y_hbm, z_hbm, yn_ref, zn_ref,
           pat_ref, keep_ref, y_ref, z_ref,
           own_y, own_z, own_t, recv, relay, bypass, cross, yh, yl, zh, zl, th, tl, rh, rl, acc_y, acc_z, acc_p,
           send_sem, recv_sem, far_send, far_recv, side_send, side_recv, relay_send, relay_recv,
           last_send, last_recv, bypass_sem, load_sem, ready):
    loads = [
        pltpu.make_async_copy(source, target, load_sem.at[i])
        for i, (source, target) in enumerate((
            (pat_hbm, pat_ref), (keep_hbm, keep_ref), (y_hbm, y_ref), (z_hbm, z_ref)))
    ]
    for load in loads:
        load.start()
    row = lax.axis_index("row")
    col = lax.axis_index("col")
    odd = lax.rem(row, 2)
    near = (row + 1 - 2 * odd, col)
    far = (lax.rem(row + row_count - 1 + 2 * odd, row_count), col)
    back = (row, lax.rem(col + col_count - 1, col_count))
    place = lax.rem(col, RUN)
    head = place == 0
    first_col = col - place
    twin_col = lax.rem(col + RUN, col_count)
    twin = (row, twin_col)
    twin_far = (far[0], twin_col)
    twin_back = (row, lax.rem(twin_col + col_count - 1, col_count))

    barrier = pltpu.get_barrier_semaphore()
    def enter(*targets):
        for target in targets:
            pl.semaphore_signal(barrier, inc=1, device_id=target, device_id_type=MESH)

    enter(far, near)

    @pl.when(head)
    def _():
        enter(twin, twin_far)
        for d in range(1, RUN):
            enter((row, col + d), (far[0], col + d))

    @pl.when(jnp.logical_and(place > 0, place < RUN - 1))
    def _():
        enter((row, col + 1))

    loads[0].wait()
    loads[1].wait()

    def first(place):
        return (place[0] * col_count + place[1]) * ROWS

    starts = [first(place) for place in ((row, col), near, far, (row, lax.rem(col + 1, col_count)))]
    labels = [pat_ref[0, starts[q // ROWS] + q % ROWS] for q in range(SLOTS)]

    def pick(wanted, keys, values):
        found = values[0]
        for key, value in zip(keys[1:], values[1:]):
            found = jnp.where(key == wanted, value, found)
        return found

    numbers = [jnp.int32(k) for k in range(SLOTS)]
    keys = [[pat_ref[k, starts[OWN] + s] for k in range(SLOTS)] for s in range(ROWS)]
    keep = [[jnp.float32(1)] + [keep_ref[k, starts[OWN] + s].astype(jnp.float32) for k in range(1, SLOTS)]
            for s in range(ROWS)]
    slot_of = [[pick(labels[q], keys[s], numbers) for q in range(SLOTS)] for s in range(ROWS)]
    place_of = [[pick(keys[s][k], labels, numbers) for k in range(SLOTS)] for s in range(ROWS)]
    kept = [[pick(labels[q], keys[s], keep[s]) for q in range(SLOTS)] for s in range(ROWS)]
    kept_far = []
    for s in range(ROWS):
        far_keys = [pat_ref[k, starts[FAR] + s] for k in range(SLOTS)]
        far_keep = [keep_ref[k, starts[FAR] + s].astype(jnp.float32) for k in range(SLOTS)]
        kept_far.append([pick(labels[e], far_keys, far_keep) for e in range(ROWS)])

    def same(value, number):
        return jnp.full((BLK, BLK), value, jnp.int32) == number

    def blk(s, e):
        return pl.ds(s * BLK, BLK), pl.ds(e * BLK, BLK)

    def arrange(load, source, whole, high, low):
        load.wait()
        for g in (FAR, OWN, NEAR, SIDE):
            for s in range(ROWS):
                for e in range(ROWS):
                    slot = slot_of[s][g * ROWS + e]
                    value = source[s, :, pl.ds(0, BLK)]
                    for k in range(1, SLOTS):
                        value = jnp.where(same(slot, k), source[s, :, pl.ds(k * BLK, BLK)], value)
                    h, l = split(value)
                    where = (g, *blk(s, e))
                    whole[where] = value
                    high[where] = h
                    low[where] = l

    arrange(loads[2], y_ref, own_y, yh, yl)
    pl.semaphore_wait(barrier, jnp.where(place > 1, 5, 4))

    @pl.when(jnp.logical_not(head))
    def _():
        pl.semaphore_signal(ready, inc=1, device_id=(row, first_col), device_id_type=MESH)

    copies = {}

    def send(source, unit, target):
        copy = pltpu.make_async_remote_copy(
            src_ref=source, dst_ref=recv.at[unit], send_sem=send_sem.at[unit],
            recv_sem=recv_sem.at[unit], device_id=target, device_id_type=MESH)
        copy.start()
        copies[unit] = copy

    def chunk(j):
        return pl.ds(j * CHUNK, CHUNK)

    def remote(source, target, send_to, recv_from, device):
        return pltpu.make_async_remote_copy(
            src_ref=source, dst_ref=target, send_sem=send_to, recv_sem=recv_from,
            device_id=device, device_id_type=MESH)

    def far_copy(source, n, j):
        return remote(source.at[chunk(j)], recv.at[FARS[n], chunk(j)], far_send.at[n, j], far_recv.at[n, j], far)

    def side_copy(source, n, j):
        return remote(source.at[chunk(j)], recv.at[SIDES[n], chunk(j)], side_send.at[n, j], side_recv.at[n, j], back)

    def far_whole(source, n):
        return remote(source, recv.at[FARS[n]], far_send.at[n, 0], far_recv.at[n, 0], far)

    def side_whole(source, n):
        return remote(source, recv.at[SIDES[n]], side_send.at[n, 0], side_recv.at[n, 0], back)

    def twin_copy(source, n, j):
        return remote(source.at[chunk(j)], relay.at[n, chunk(j)], far_send.at[n, j], relay_recv.at[n, j], twin)

    def on_far(n, j):
        return remote(relay.at[n, chunk(j)], recv.at[FARS[n], chunk(j)], relay_send.at[n, j], far_recv.at[n, j], twin_far)

    def on_side(n, j):
        return remote(relay.at[n, chunk(j)], recv.at[SIDES[n], chunk(j)], side_send.at[n, j], side_recv.at[n, j], twin_back)

    def send_own(source, n):
        @pl.when(head)
        def _():
            for j in range(PARTS):
                twin_copy(source, n, j).start()

        @pl.when(jnp.logical_not(head))
        def _():
            far_whole(source, n).start()
            side_whole(source, n).start()

    def pass_on(n, chunks=range(PARTS)):
        @pl.when(head)
        def _():
            for j in chunks:
                twin_copy(own_y.at[OWN], n, j).wait_recv()
                on_far(n, j).start()
                on_side(n, j).start()

    def carried(j):
        return pl.ds(pl.multiple_of(UNIT - (RUN - j) * CARRY, 8), CARRY)

    def last_rows(j):
        return carried(j) if j else pl.ds(0, UNIT - (RUN - 1) * CARRY)

    def last_copy(j):
        return remote(own_z.at[FAR, last_rows(j)], recv.at[Z_XO, last_rows(j)], last_send.at[j], last_recv.at[j], far)

    def detour_copy(j):
        return remote(own_z.at[FAR, carried(j)], bypass, last_send.at[j], bypass_sem.at[0], (row, col + j))

    def on_detour():
        return remote(bypass, recv.at[Z_XO, carried(place)], bypass_sem.at[1], last_recv.at[place], (far[0], first_col))

    def send_last_direct():
        @pl.when(jnp.logical_not(head))
        def _():
            for j in range(RUN):
                last_copy(j).start()

    def send_last_detour():
        @pl.when(head)
        def _():
            pl.semaphore_wait(ready, RUN - 1)
            for j in range(1, RUN):
                detour_copy(j).start()

    def pass_detour():
        @pl.when(jnp.logical_not(head))
        def _():
            detour_copy(1).wait_recv()
            on_detour().start()

    send(own_y.at[FAR], Y_XO, far)
    send_own(own_y.at[OWN], 0)
    send(own_y.at[NEAR], Y_NO, near)
    send(own_y.at[OWN], Y_NN, near)
    arrange(loads[3], z_ref, own_z, zh, zl)
    send_own(own_z.at[OWN], 1)
    send(own_z.at[NEAR], Z_NO, near)
    send(own_z.at[OWN], Z_NN, near)

    def arrive(unit):
        if unit in SIDES:
            @pl.when(place == RUN - 1)
            def _():
                for j in range(PARTS):
                    side_copy(own_y.at[OWN], SIDES.index(unit), j).wait_recv()

            @pl.when(place != RUN - 1)
            def _():
                side_whole(own_y.at[OWN], SIDES.index(unit)).wait_recv()
        elif unit in FARS:
            @pl.when(head)
            def _():
                for j in range(PARTS):
                    far_copy(own_y.at[OWN], FARS.index(unit), j).wait_recv()

            @pl.when(jnp.logical_not(head))
            def _():
                far_whole(own_y.at[OWN], FARS.index(unit)).wait_recv()
        else:
            copies[unit].wait_recv()
        h, l = split(recv[unit])
        rh[unit] = h
        rl[unit] = l

    def mul(a_high, a_low, b_high, b_low):
        dot = functools.partial(jnp.dot, preferred_element_type=jnp.float32)
        return dot(a_high, b_high) + (dot(a_high, b_low) + dot(a_low, b_high))

    Y = lambda g: (yh[g], yl[g])
    Z = lambda g: (zh[g], zl[g])
    T = lambda g: (th[g], tl[g])
    R = lambda u: (rh[u], rl[u])

    def factor_of(product, region, s, e):
        value = (-0.5 * kept[s][region * ROWS + e]) * product[s * BLK:(s + 1) * BLK, e * BLK:(e + 1) * BLK]
        if region == OWN and s == e:
            eye = lax.broadcasted_iota(jnp.int32, (BLK, BLK), 0) == lax.broadcasted_iota(jnp.int32, (BLK, BLK), 1)
            value = value + jnp.where(eye, jnp.float32(1.5), jnp.float32(0))
        return value

    def set_factor(region, product):
        for s in range(ROWS):
            for e in range(ROWS):
                value = factor_of(product, region, s, e)
                h, l = split(value)
                where = (region, *blk(s, e))
                th[where] = h
                tl[where] = l
                if region in (OWN, NEAR):
                    own_t[where] = value

    def parts(g):
        return [(g * ROWS + e, s, blk_of(s, e)) for s in range(ROWS) for e in range(ROWS)]

    def blk_of(s, e):
        return slice(s * BLK, (s + 1) * BLK), slice(e * BLK, (e + 1) * BLK)

    def put(acc, g, value):
        for q, s, where in parts(g):
            acc[q, s] = value[where]

    def add(acc, g, value):
        for q, s, where in parts(g):
            acc[q, s] += value[where]

    def get(acc, g):
        rows = [jnp.concatenate([acc[g * ROWS + e, s] for e in range(ROWS)], axis=1) for s in range(ROWS)]
        return jnp.concatenate(rows, axis=0)

    arrive(Y_NO)
    put(acc_z, OWN, mul(*Z(OWN), *Y(OWN)) + mul(*Z(NEAR), *R(Y_NO)))
    arrive(Y_NN)
    set_factor(NEAR, mul(*Z(OWN), *Y(NEAR)) + mul(*Z(NEAR), *R(Y_NN)))
    send(own_t.at[NEAR], T_NO, near)
    put(acc_p, FAR, mul(*Z(OWN), *Y(FAR)))
    put(acc_p, SIDE, mul(*Z(OWN), *Y(SIDE)))
    put(acc_y, NEAR, mul(*Y(OWN), *T(NEAR)))
    send_last_detour()
    pass_detour()
    pass_on(0)
    arrive(Y_XO)
    set_factor(OWN, get(acc_z, OWN) + mul(*Z(FAR), *R(Y_XO)))
    @pl.when(head)
    def _():
        last_copy(0).start()

    send_own(own_t.at[OWN], 2)
    send(own_t.at[OWN], T_NN, near)
    send_last_direct()
    pass_on(1, range(0, 1))
    arrive(Z_NO)
    arrive(Z_NN)
    put(acc_y, OWN, mul(*Y(OWN), *T(OWN)))
    put(acc_z, OWN, mul(*T(OWN), *Z(OWN)) + mul(*T(NEAR), *R(Z_NO)))
    pass_on(1, range(1, 2))
    put(acc_z, NEAR, mul(*T(OWN), *Z(NEAR)) + mul(*T(NEAR), *R(Z_NN)))
    arrive(T_NO)
    add(acc_y, OWN, mul(*Y(NEAR), *R(T_NO)))
    pass_on(1, range(2, 3))
    arrive(T_NN)
    add(acc_y, NEAR, mul(*Y(NEAR), *R(T_NN)))
    put(acc_z, FAR, mul(*T(OWN), *Z(FAR)))
    put(acc_z, SIDE, mul(*T(OWN), *Z(SIDE)))
    pass_on(1, range(3, 4))
    arrive(Y_XX)
    set_factor(FAR, get(acc_p, FAR) + mul(*Z(FAR), *R(Y_XX)))
    put(acc_y, FAR, mul(*Y(OWN), *T(FAR)))
    pass_on(2, range(0, 1))
    arrive(Y_SS)
    set_factor(SIDE, get(acc_p, SIDE) + mul(*Z(SIDE), *R(Y_SS)))
    put(acc_y, SIDE, mul(*Y(OWN), *T(SIDE)))
    pass_on(2, range(1, PARTS))
    arrive(Z_XX)
    add(acc_z, FAR, mul(*T(FAR), *R(Z_XX)))
    arrive(Z_SS)
    add(acc_z, SIDE, mul(*T(SIDE), *R(Z_SS)))
    cross[...] = mul(*R(Z_XX), *R(Y_XO))
    arrive(T_SS)
    add(acc_y, SIDE, mul(*Y(SIDE), *R(T_SS)))
    arrive(T_XX)
    add(acc_y, FAR, mul(*Y(FAR), *R(T_XX)))
    for s in range(ROWS):
        for j in ((0,), range(1, RUN))[s]:
            last_copy(j).wait_recv()
        rows = pl.ds(s * HALF, HALF)
        high, low = split(recv[Z_XO, rows])
        add(acc_z, OWN, mul(th[FAR, :, rows], tl[FAR, :, rows], high, low))
        value = cross[rows] + mul(high, low, *Y(OWN))
        value = -0.5 * jnp.concatenate(
            [kept_far[s][e] * value[:, e * BLK:(e + 1) * BLK] for e in range(ROWS)], axis=1)
        high, low = split(value)
        add(acc_y, OWN, mul(yh[FAR, :, rows], yl[FAR, :, rows], high, low))

    def emit(result, out):
        for s in range(ROWS):
            for p in range(SLOTS):
                out[s, :, pl.ds(p * BLK, BLK)] = keep[s][p] * result[place_of[s][p], s]

    emit(acc_z, zn_ref)
    emit(acc_y, yn_ref)
    for copy in copies.values():
        copy.wait_send()
    for j in range(RUN):
        last_copy(j).wait_send()

    @pl.when(head)
    def _():
        for n in range(len(FARS)):
            for j in range(PARTS):
                twin_copy(own_y.at[OWN], n, j).wait_send()
                on_far(n, j).wait_send()
                on_side(n, j).wait_send()

    @pl.when(jnp.logical_not(head))
    def _():
        for n in range(len(FARS)):
            far_whole(own_y.at[OWN], n).wait_send()
            side_whole(own_y.at[OWN], n).wait_send()
        on_detour().wait_send()


def write_out(y_ref, z_ref, y_hbm, z_hbm, sem):
    copies = []
    for source, target in ((y_ref, y_hbm), (z_ref, z_hbm)):
        for s in range(ROWS):
            for part in range(2):
                where = (s, pl.ds(part * (BLK // 2), BLK // 2))
                copies.append(pltpu.make_async_copy(source.at[where], target.at[where], sem.at[len(copies)]))
    for copy in copies:
        copy.start()
    for copy in copies:
        copy.wait()


def local(row_count, col_count, sqrt_iterate, inverse_iterate, pattern, keep_mask, row_order):
    del row_order
    whole = jax.ShapeDtypeStruct(sqrt_iterate.shape, jnp.float32)
    unit = (UNIT, UNIT)
    vmem = pl.BlockSpec(memory_space=pltpu.VMEM)
    f32 = lambda n: pltpu.VMEM((n, *unit), jnp.float32)
    b16 = lambda n: pltpu.VMEM((n, *unit), jnp.bfloat16)
    hbm = pl.BlockSpec(memory_space=pltpu.HBM)
    stay = lambda array: pltpu.with_memory_space_constraint(array, pltpu.HBM)
    dma = pltpu.SemaphoreType.DMA
    results = pl.pallas_call(
        functools.partial(kernel, row_count, col_count),
        out_shape=(whole, whole),
        in_specs=[hbm] * 4,
        out_specs=(vmem, vmem),
        scratch_shapes=[
            pltpu.SMEM(pattern.shape[::-1], jnp.int32), pltpu.SMEM(pattern.shape[::-1], jnp.int32),
            pltpu.VMEM(whole.shape, jnp.float32), pltpu.VMEM(whole.shape, jnp.float32),
            f32(4), f32(4), f32(2), f32(14), f32(3), pltpu.VMEM((CARRY, UNIT), jnp.float32), pltpu.VMEM(unit, jnp.float32),
            b16(4), b16(4), b16(4), b16(4), b16(4), b16(4), b16(14), b16(14),
            pltpu.VMEM((SLOTS, ROWS, BLK, BLK), jnp.float32),
            pltpu.VMEM((SLOTS, ROWS, BLK, BLK), jnp.float32),
            pltpu.VMEM((SLOTS, ROWS, BLK, BLK), jnp.float32),
            dma((14,)), dma((14,)), *[dma((3, PARTS))] * 6, dma((RUN,)), dma((RUN,)), dma((2,)), dma((4,)), pltpu.SemaphoreType.REGULAR,
        ],
        compiler_params=pltpu.CompilerParams(
            collective_id=0, has_side_effects=True, vmem_limit_bytes=54_000_000),
    )(*map(stay, (pattern.T, keep_mask.T, sqrt_iterate, inverse_iterate)))
    return pl.pallas_call(
        write_out,
        out_shape=(whole, whole),
        in_specs=[vmem, vmem],
        out_specs=(hbm, hbm),
        scratch_shapes=[dma((8,))],
        compiler_params=pltpu.CompilerParams(vmem_limit_bytes=4194304),
    )(*results)


def solution(mesh):
    split_rows = P(("row", "col"), None, None)
    body = functools.partial(local, mesh.shape["row"], mesh.shape["col"])
    return jax.shard_map(
        body, mesh=mesh, in_specs=(split_rows, split_rows, P(), P(), P()),
        out_specs=(split_rows, split_rows), check_vma=False)
```

```python
import functools

import jax
import jax.numpy as jnp
from jax import lax
from jax.experimental import pallas as pl
from jax.experimental.pallas import tpu as pltpu
from jax.sharding import PartitionSpec as P

MESH = pl.DeviceIdType.MESH
BLK = 128
ROWS = 2
SLOTS = 8
UNIT = ROWS * BLK

OWN, NEAR, FAR, SIDE = 0, 1, 2, 3

RUN = 4
PARTS = 4
CHUNK = UNIT // PARTS
HALF = UNIT // 2
CARRY = 40
assert UNIT - (RUN - 1) * CARRY >= HALF

(Y_NO, Y_NN, Z_NO, Z_NN, T_NO, T_NN,
 Y_XO, Y_XX, Z_XO, Z_XX, T_XX,
 Y_SS, Z_SS, T_SS) = range(14)
SIDES = (Y_SS, Z_SS, T_SS)
FARS = (Y_XX, Z_XX, T_XX)


def split(value):
    high = value.astype(jnp.bfloat16)
    low = (value - high.astype(jnp.float32)).astype(jnp.bfloat16)
    return high, low


def kernel(row_count, col_count, pat_hbm, keep_hbm, y_hbm, z_hbm, yn_ref, zn_ref,
           pat_ref, keep_ref, y_ref, z_ref,
           own_y, own_z, own_t, recv, relay, bypass, cross, yh, yl, zh, zl, th, tl, rh, rl, acc_y, acc_z, acc_p,
           send_sem, recv_sem, far_send, far_recv, side_send, side_recv, relay_send, relay_recv,
           last_send, last_recv, bypass_sem, load_sem, ready):
    loads = [
        pltpu.make_async_copy(source, target, load_sem.at[i])
        for i, (source, target) in enumerate((
            (pat_hbm, pat_ref), (keep_hbm, keep_ref), (y_hbm, y_ref), (z_hbm, z_ref)))
    ]
    row = lax.axis_index("row")
    col = lax.axis_index("col")
    odd = lax.rem(row, 2)
    near = (row + 1 - 2 * odd, col)
    far = (lax.rem(row + row_count - 1 + 2 * odd, row_count), col)
    back = (row, lax.rem(col + col_count - 1, col_count))
    place = lax.rem(col, RUN)
    head = place == 0
    first_col = col - place
    twin_col = lax.rem(col + RUN, col_count)
    twin = (row, twin_col)
    twin_far = (far[0], twin_col)
    twin_back = (row, lax.rem(twin_col + col_count - 1, col_count))

    barrier = pltpu.get_barrier_semaphore()
    def enter(*targets):
        for target in targets:
            pl.semaphore_signal(barrier, inc=1, device_id=target, device_id_type=MESH)

    enter(far, near)

    @pl.when(head)
    def _():
        enter(twin, twin_far)
        for d in range(1, RUN):
            enter((row, col + d), (far[0], col + d))

    @pl.when(jnp.logical_and(place > 0, place < RUN - 1))
    def _():
        enter((row, col + 1))

    for load in loads:
        load.start()
    loads[0].wait()
    loads[1].wait()

    def first(place):
        return (place[0] * col_count + place[1]) * ROWS

    starts = [first(place) for place in ((row, col), near, far, (row, lax.rem(col + 1, col_count)))]
    labels = [pat_ref[0, starts[q // ROWS] + q % ROWS] for q in range(SLOTS)]

    def pick(wanted, keys, values):
        found = values[0]
        for key, value in zip(keys[1:], values[1:]):
            found = jnp.where(key == wanted, value, found)
        return found

    numbers = [jnp.int32(k) for k in range(SLOTS)]
    keys = [[pat_ref[k, starts[OWN] + s] for k in range(SLOTS)] for s in range(ROWS)]
    keep = [[jnp.float32(1)] + [keep_ref[k, starts[OWN] + s].astype(jnp.float32) for k in range(1, SLOTS)]
            for s in range(ROWS)]
    slot_of = [[pick(labels[q], keys[s], numbers) for q in range(SLOTS)] for s in range(ROWS)]
    place_of = [[pick(keys[s][k], labels, numbers) for k in range(SLOTS)] for s in range(ROWS)]
    kept = [[pick(labels[q], keys[s], keep[s]) for q in range(SLOTS)] for s in range(ROWS)]
    kept_far = []
    for s in range(ROWS):
        far_keys = [pat_ref[k, starts[FAR] + s] for k in range(SLOTS)]
        far_keep = [keep_ref[k, starts[FAR] + s].astype(jnp.float32) for k in range(SLOTS)]
        kept_far.append([pick(labels[e], far_keys, far_keep) for e in range(ROWS)])

    def same(value, number):
        return jnp.full((BLK, BLK), value, jnp.int32) == number

    def blk(s, e):
        return pl.ds(s * BLK, BLK), pl.ds(e * BLK, BLK)

    def arrange(load, source, whole, high, low):
        load.wait()
        for g in (FAR, OWN, NEAR, SIDE):
            for s in range(ROWS):
                for e in range(ROWS):
                    slot = slot_of[s][g * ROWS + e]
                    value = source[s, :, pl.ds(0, BLK)]
                    for k in range(1, SLOTS):
                        value = jnp.where(same(slot, k), source[s, :, pl.ds(k * BLK, BLK)], value)
                    h, l = split(value)
                    where = (g, *blk(s, e))
                    whole[where] = value
                    high[where] = h
                    low[where] = l

    arrange(loads[2], y_ref, own_y, yh, yl)
    pl.semaphore_wait(barrier, jnp.where(place > 1, 5, 4))

    @pl.when(jnp.logical_not(head))
    def _():
        pl.semaphore_signal(ready, inc=1, device_id=(row, first_col), device_id_type=MESH)

    copies = {}

    def send(source, unit, target):
        copy = pltpu.make_async_remote_copy(
            src_ref=source, dst_ref=recv.at[unit], send_sem=send_sem.at[unit],
            recv_sem=recv_sem.at[unit], device_id=target, device_id_type=MESH)
        copy.start()
        copies[unit] = copy

    def chunk(j):
        return pl.ds(j * CHUNK, CHUNK)

    def remote(source, target, send_to, recv_from, device):
        return pltpu.make_async_remote_copy(
            src_ref=source, dst_ref=target, send_sem=send_to, recv_sem=recv_from,
            device_id=device, device_id_type=MESH)

    def far_copy(source, n, j):
        return remote(source.at[chunk(j)], recv.at[FARS[n], chunk(j)], far_send.at[n, j], far_recv.at[n, j], far)

    def side_copy(source, n, j):
        return remote(source.at[chunk(j)], recv.at[SIDES[n], chunk(j)], side_send.at[n, j], side_recv.at[n, j], back)

    def far_whole(source, n):
        return remote(source, recv.at[FARS[n]], far_send.at[n, 0], far_recv.at[n, 0], far)

    def side_whole(source, n):
        return remote(source, recv.at[SIDES[n]], side_send.at[n, 0], side_recv.at[n, 0], back)

    def twin_copy(source, n, j):
        return remote(source.at[chunk(j)], relay.at[n, chunk(j)], far_send.at[n, j], relay_recv.at[n, j], twin)

    def on_far(n, j):
        return remote(relay.at[n, chunk(j)], recv.at[FARS[n], chunk(j)], relay_send.at[n, j], far_recv.at[n, j], twin_far)

    def on_side(n, j):
        return remote(relay.at[n, chunk(j)], recv.at[SIDES[n], chunk(j)], side_send.at[n, j], side_recv.at[n, j], twin_back)

    def send_own(source, n):
        @pl.when(head)
        def _():
            for j in range(PARTS):
                twin_copy(source, n, j).start()

        @pl.when(jnp.logical_not(head))
        def _():
            far_whole(source, n).start()
            side_whole(source, n).start()

    def pass_on(n, chunks=range(PARTS)):
        @pl.when(head)
        def _():
            for j in chunks:
                twin_copy(own_y.at[OWN], n, j).wait_recv()
                on_far(n, j).start()
                on_side(n, j).start()

    def carried(j):
        return pl.ds(pl.multiple_of(UNIT - (RUN - j) * CARRY, 8), CARRY)

    def last_rows(j):
        return carried(j) if j else pl.ds(0, UNIT - (RUN - 1) * CARRY)

    def last_copy(j):
        return remote(own_z.at[FAR, last_rows(j)], recv.at[Z_XO, last_rows(j)], last_send.at[j], last_recv.at[j], far)

    def detour_copy(j):
        return remote(own_z.at[FAR, carried(j)], bypass, last_send.at[j], bypass_sem.at[0], (row, col + j))

    def on_detour():
        return remote(bypass, recv.at[Z_XO, carried(place)], bypass_sem.at[1], last_recv.at[place], (far[0], first_col))

    def send_last_direct():
        @pl.when(jnp.logical_not(head))
        def _():
            for j in range(RUN):
                last_copy(j).start()

    def send_last_detour():
        @pl.when(head)
        def _():
            pl.semaphore_wait(ready, RUN - 1)
            for j in range(1, RUN):
                detour_copy(j).start()

    def pass_detour():
        @pl.when(jnp.logical_not(head))
        def _():
            detour_copy(1).wait_recv()
            on_detour().start()

    send(own_y.at[FAR], Y_XO, far)
    send_own(own_y.at[OWN], 0)
    send(own_y.at[NEAR], Y_NO, near)
    send(own_y.at[OWN], Y_NN, near)
    arrange(loads[3], z_ref, own_z, zh, zl)
    send_own(own_z.at[OWN], 1)
    send(own_z.at[NEAR], Z_NO, near)
    send(own_z.at[OWN], Z_NN, near)

    def arrive(unit):
        if unit in SIDES:
            @pl.when(place == RUN - 1)
            def _():
                for j in range(PARTS):
                    side_copy(own_y.at[OWN], SIDES.index(unit), j).wait_recv()

            @pl.when(place != RUN - 1)
            def _():
                side_whole(own_y.at[OWN], SIDES.index(unit)).wait_recv()
        elif unit in FARS:
            @pl.when(head)
            def _():
                for j in range(PARTS):
                    far_copy(own_y.at[OWN], FARS.index(unit), j).wait_recv()

            @pl.when(jnp.logical_not(head))
            def _():
                far_whole(own_y.at[OWN], FARS.index(unit)).wait_recv()
        else:
            copies[unit].wait_recv()
        h, l = split(recv[unit])
        rh[unit] = h
        rl[unit] = l

    def mul(a_high, a_low, b_high, b_low):
        dot = functools.partial(jnp.dot, preferred_element_type=jnp.float32)
        return dot(a_high, b_high) + (dot(a_high, b_low) + dot(a_low, b_high))

    Y = lambda g: (yh[g], yl[g])
    Z = lambda g: (zh[g], zl[g])
    T = lambda g: (th[g], tl[g])
    R = lambda u: (rh[u], rl[u])

    def factor_of(product, region, s, e):
        value = (-0.5 * kept[s][region * ROWS + e]) * product[s * BLK:(s + 1) * BLK, e * BLK:(e + 1) * BLK]
        if region == OWN and s == e:
            eye = lax.broadcasted_iota(jnp.int32, (BLK, BLK), 0) == lax.broadcasted_iota(jnp.int32, (BLK, BLK), 1)
            value = value + jnp.where(eye, jnp.float32(1.5), jnp.float32(0))
        return value

    def set_factor(region, product):
        for s in range(ROWS):
            for e in range(ROWS):
                value = factor_of(product, region, s, e)
                h, l = split(value)
                where = (region, *blk(s, e))
                th[where] = h
                tl[where] = l
                if region in (OWN, NEAR):
                    own_t[where] = value

    def parts(g):
        return [(g * ROWS + e, s, blk_of(s, e)) for s in range(ROWS) for e in range(ROWS)]

    def blk_of(s, e):
        return slice(s * BLK, (s + 1) * BLK), slice(e * BLK, (e + 1) * BLK)

    def put(acc, g, value):
        for q, s, where in parts(g):
            acc[q, s] = value[where]

    def add(acc, g, value):
        for q, s, where in parts(g):
            acc[q, s] += value[where]

    def get(acc, g):
        rows = [jnp.concatenate([acc[g * ROWS + e, s] for e in range(ROWS)], axis=1) for s in range(ROWS)]
        return jnp.concatenate(rows, axis=0)

    arrive(Y_NO)
    put(acc_z, OWN, mul(*Z(OWN), *Y(OWN)) + mul(*Z(NEAR), *R(Y_NO)))
    arrive(Y_NN)
    set_factor(NEAR, mul(*Z(OWN), *Y(NEAR)) + mul(*Z(NEAR), *R(Y_NN)))
    send(own_t.at[NEAR], T_NO, near)
    put(acc_p, FAR, mul(*Z(OWN), *Y(FAR)))
    put(acc_p, SIDE, mul(*Z(OWN), *Y(SIDE)))
    put(acc_y, NEAR, mul(*Y(OWN), *T(NEAR)))
    send_last_detour()
    pass_detour()
    pass_on(0)
    arrive(Y_XO)
    set_factor(OWN, get(acc_z, OWN) + mul(*Z(FAR), *R(Y_XO)))
    @pl.when(head)
    def _():
        last_copy(0).start()

    send_own(own_t.at[OWN], 2)
    send(own_t.at[OWN], T_NN, near)
    send_last_direct()
    pass_on(1, range(0, 1))
    arrive(Z_NO)
    arrive(Z_NN)
    put(acc_y, OWN, mul(*Y(OWN), *T(OWN)))
    put(acc_z, OWN, mul(*T(OWN), *Z(OWN)) + mul(*T(NEAR), *R(Z_NO)))
    pass_on(1, range(1, 2))
    put(acc_z, NEAR, mul(*T(OWN), *Z(NEAR)) + mul(*T(NEAR), *R(Z_NN)))
    arrive(T_NO)
    add(acc_y, OWN, mul(*Y(NEAR), *R(T_NO)))
    pass_on(1, range(2, 3))
    arrive(T_NN)
    add(acc_y, NEAR, mul(*Y(NEAR), *R(T_NN)))
    put(acc_z, FAR, mul(*T(OWN), *Z(FAR)))
    put(acc_z, SIDE, mul(*T(OWN), *Z(SIDE)))
    pass_on(1, range(3, 4))
    arrive(Y_XX)
    set_factor(FAR, get(acc_p, FAR) + mul(*Z(FAR), *R(Y_XX)))
    put(acc_y, FAR, mul(*Y(OWN), *T(FAR)))
    pass_on(2, range(0, 1))
    arrive(Y_SS)
    set_factor(SIDE, get(acc_p, SIDE) + mul(*Z(SIDE), *R(Y_SS)))
    put(acc_y, SIDE, mul(*Y(OWN), *T(SIDE)))
    pass_on(2, range(1, PARTS))
    arrive(Z_XX)
    add(acc_z, FAR, mul(*T(FAR), *R(Z_XX)))
    arrive(Z_SS)
    add(acc_z, SIDE, mul(*T(SIDE), *R(Z_SS)))
    cross[...] = mul(*R(Z_XX), *R(Y_XO))
    arrive(T_SS)
    add(acc_y, SIDE, mul(*Y(SIDE), *R(T_SS)))
    arrive(T_XX)
    add(acc_y, FAR, mul(*Y(FAR), *R(T_XX)))
    for s in range(ROWS):
        for j in ((0,), range(1, RUN))[s]:
            last_copy(j).wait_recv()
        rows = pl.ds(s * HALF, HALF)
        high, low = split(recv[Z_XO, rows])
        add(acc_z, OWN, mul(th[FAR, :, rows], tl[FAR, :, rows], high, low))
        value = cross[rows] + mul(high, low, *Y(OWN))
        value = -0.5 * jnp.concatenate(
            [kept_far[s][e] * value[:, e * BLK:(e + 1) * BLK] for e in range(ROWS)], axis=1)
        high, low = split(value)
        add(acc_y, OWN, mul(yh[FAR, :, rows], yl[FAR, :, rows], high, low))

    def emit(result, out):
        for s in range(ROWS):
            for p in range(SLOTS):
                out[s, :, pl.ds(p * BLK, BLK)] = keep[s][p] * result[place_of[s][p], s]

    emit(acc_z, zn_ref)
    emit(acc_y, yn_ref)
    for copy in copies.values():
        copy.wait_send()
    for j in range(RUN):
        last_copy(j).wait_send()

    @pl.when(head)
    def _():
        for n in range(len(FARS)):
            for j in range(PARTS):
                twin_copy(own_y.at[OWN], n, j).wait_send()
                on_far(n, j).wait_send()
                on_side(n, j).wait_send()

    @pl.when(jnp.logical_not(head))
    def _():
        for n in range(len(FARS)):
            far_whole(own_y.at[OWN], n).wait_send()
            side_whole(own_y.at[OWN], n).wait_send()
        on_detour().wait_send()


def write_out(y_ref, z_ref, y_hbm, z_hbm, sem):
    copies = []
    for source, target in ((y_ref, y_hbm), (z_ref, z_hbm)):
        for s in range(ROWS):
            copies.append(pltpu.make_async_copy(source.at[s], target.at[s], sem.at[len(copies)]))
    for copy in copies:
        copy.start()
    for copy in copies:
        copy.wait()


def local(row_count, col_count, sqrt_iterate, inverse_iterate, pattern, keep_mask, row_order):
    del row_order
    whole = jax.ShapeDtypeStruct(sqrt_iterate.shape, jnp.float32)
    unit = (UNIT, UNIT)
    vmem = pl.BlockSpec(memory_space=pltpu.VMEM)
    f32 = lambda n: pltpu.VMEM((n, *unit), jnp.float32)
    b16 = lambda n: pltpu.VMEM((n, *unit), jnp.bfloat16)
    hbm = pl.BlockSpec(memory_space=pltpu.HBM)
    stay = lambda array: pltpu.with_memory_space_constraint(array, pltpu.HBM)
    dma = pltpu.SemaphoreType.DMA
    results = pl.pallas_call(
        functools.partial(kernel, row_count, col_count),
        out_shape=(whole, whole),
        in_specs=[hbm] * 4,
        out_specs=(vmem, vmem),
        scratch_shapes=[
            pltpu.SMEM(pattern.shape[::-1], jnp.int32), pltpu.SMEM(pattern.shape[::-1], jnp.int32),
            pltpu.VMEM(whole.shape, jnp.float32), pltpu.VMEM(whole.shape, jnp.float32),
            f32(4), f32(4), f32(2), f32(14), f32(3), pltpu.VMEM((CARRY, UNIT), jnp.float32), pltpu.VMEM(unit, jnp.float32),
            b16(4), b16(4), b16(4), b16(4), b16(4), b16(4), b16(14), b16(14),
            pltpu.VMEM((SLOTS, ROWS, BLK, BLK), jnp.float32),
            pltpu.VMEM((SLOTS, ROWS, BLK, BLK), jnp.float32),
            pltpu.VMEM((SLOTS, ROWS, BLK, BLK), jnp.float32),
            dma((14,)), dma((14,)), *[dma((3, PARTS))] * 6, dma((RUN,)), dma((RUN,)), dma((2,)), dma((4,)), pltpu.SemaphoreType.REGULAR,
        ],
        compiler_params=pltpu.CompilerParams(
            collective_id=0, has_side_effects=True, vmem_limit_bytes=54_000_000),
    )(*map(stay, (pattern.T, keep_mask.T, sqrt_iterate, inverse_iterate)))
    return pl.pallas_call(
        write_out,
        out_shape=(whole, whole),
        in_specs=[vmem, vmem],
        out_specs=(hbm, hbm),
        scratch_shapes=[dma((4,))],
        compiler_params=pltpu.CompilerParams(vmem_limit_bytes=4194304),
    )(*results)


def solution(mesh):
    split_rows = P(("row", "col"), None, None)
    body = functools.partial(local, mesh.shape["row"], mesh.shape["col"])
    return jax.shard_map(
        body, mesh=mesh, in_specs=(split_rows, split_rows, P(), P(), P()),
        out_specs=(split_rows, split_rows), check_vma=False)
```
